32 devices in a mesh: band: 8 (over z, x), sub: 4 (over y, core).
Axes of the slice: x: 2, y: 2, z: 4, core: 2. Of those that a mesh axis runs over, the one named last changes fastest.
Arguments:
- grad_pred: bfloat16 [227, 24576], P(None, ('band', 'sub')), may hold values from -6 to 6
- grid_latent: bfloat16 [24576, 512], P(('band', 'sub')), may hold values from -6 to 6
- mesh_latent: bfloat16 [10240, 512], P(('band', 'sub')), may hold values from -6 to 6
- send_slot: int32 [24576], P(('band', 'sub')), may hold values from 0 to 2303, as said below
- edge_src: int32 [3, 73728], P(None, ('band', 'sub')), may hold values from 0 to 10239, as said below
- w_mesh: bfloat16 [512, 512], replicated, may hold values from -0.25 to 0.25
- w_grid: bfloat16 [512, 512], replicated, may hold values from -0.25 to 0.25
- w_msg: bfloat16 [512, 512], replicated, may hold values from -0.25 to 0.25
- w_out: bfloat16 [512, 227], replicated, may hold values from -0.25 to 0.25
Outputs:
- mesh_grad: bfloat16 [10240, 512], P(('band', 'sub'))
- grad_w_mesh: float32 [512, 512], replicated
- grad_w_grid: float32 [512, 512], replicated
- grad_w_msg: float32 [512, 512], replicated
- grad_w_out: float32 [512, 227], replicated
The draws below stay inside these ranges and needn't reach their ends.
Inputs may be any that keep to these rules, and one draw needn't show every extreme that they name: For grid point p on latitude-major device i, send_slot[p] = j * 72 + r names patch-major device j and a rank r. On one device i the values are distinct, and for each j the ranks used are 0 to the count of i's points sent to j minus 1. Every such count is at most 72, and 72 is reached in every draw. Every grid point thereby gets one patch-major slot; live slots of each source stand at the front of its block of 72. One patch-major device holds at most 1920 live slots, reached on some device in every draw. `edge_src`: A slot on patch-major device j, of band b = j // 4, names senders in patch b only: mesh rows b * 1280 to (b + 1) * 1280 - 1. Entries of empty slots lie in that range too and are not read.
All inputs are finite; a program needn't handle non-finite values.
Results may differ from the reference program's by a relative error of at most 0.0076.
Values may be sent and summed in bfloat16 or wider, within the bound.
A program may use at most 128 MiB of HBM per device.

```python
import math
import jax
import jax.numpy as jnp

D = 512
C = 227
G_DEV = 768
GRID = 24576
MESH = 10240
PATCH = 1280
CAP = 72
SLOT_DEV = 2304
SLOTS = 73728
N_BAND = 8
N_SUB = 4
DEVICES = 32


def relay_table(key):
    base_count = G_DEV // DEVICES
    half_base = base_count // 2
    receivers = jnp.arange(DEVICES, dtype=jnp.int32)
    band_index = receivers // N_SUB
    polar_band = (band_index < N_BAND // 8) | (band_index >= N_BAND - N_BAND // 8)
    receive_load = jnp.where(polar_band, 5 * half_base, half_base).astype(jnp.int32)
    draw_key, shuffle_key = jax.random.split(jax.random.fold_in(key, 7))
    increments = jax.random.randint(draw_key, (DEVICES,), 0, half_base + 1)
    increments = increments.at[0].set(half_base).at[DEVICES - 1].set(0)
    offsets = (increments - jnp.roll(increments, 1)).astype(jnp.int32)
    senders = jnp.arange(DEVICES, dtype=jnp.int32)
    counts = receive_load[None, :] + offsets[(receivers[None, :] - senders[:, None]) % DEVICES]
    block_ends = jnp.cumsum(counts, axis=1)
    starts = block_ends - counts
    positions = jnp.arange(G_DEV, dtype=jnp.int32)

    def one_sender(row_ends, row_starts, sub_key):
        target = jnp.sum((row_ends[None, :] <= positions[:, None]).astype(jnp.int32), axis=1)
        slot_rank = positions - row_starts[target]
        shuffle = jax.random.permutation(sub_key, G_DEV)
        return jnp.zeros((G_DEV,), jnp.int32).at[shuffle].set(target * CAP + slot_rank)
    sender_keys = jax.random.split(shuffle_key, DEVICES)
    table = jax.vmap(one_sender)(block_ends, starts, sender_keys)
    return table.reshape(GRID).astype(jnp.int32)


def draw_send_slot(key, part):
    return relay_table(key)


def draw_edge_src(key, part):
    local_node = jax.random.randint(jax.random.fold_in(key, 11), (3, SLOTS), 0, PATCH)
    holders = jnp.arange(SLOTS, dtype=jnp.int32) // SLOT_DEV
    band_index = holders // N_SUB
    return (local_node + band_index[None, :] * PATCH).astype(jnp.int32)


def steps_of(rng, shape, cuts, low, largest):
    def one(dim, blocks):
        steps = jax.random.uniform(jax.random.fold_in(jax.random.fold_in(rng, 6), dim), (blocks,), jnp.float32, low / len(cuts), largest / len(cuts))
        return jnp.repeat(jnp.exp(steps), shape[dim] // blocks).reshape((-1,) + (1,) * (len(shape) - dim - 1))

    loudness = one(*cuts[0])
    for cut in cuts[1:]:
        loudness = loudness * one(*cut)
    return loudness


def bell_draw(rng, dims, scale, bound, cuts=(), kind=jnp.bfloat16):
    factor_of = steps_of(rng, dims, cuts, -0.22, 0.18) if cuts else 1.0
    values = jax.random.normal(rng, dims, jnp.float32) * scale * factor_of
    return jnp.minimum(jnp.maximum(values, -bound), bound).astype(kind)


def setup_inputs(seed: int = 0) -> dict:
    seeds = jax.random.split(jax.random.key(seed), 10)
    grad_pred = bell_draw(seeds[0], (C, GRID), 1.0, 6.0, ((1, 32),))
    grid_latent = bell_draw(seeds[1], (GRID, D), 1.0, 6.0, ((0, 32),))
    mesh_latent = bell_draw(seeds[2], (MESH, D), 1.0, 6.0, ((0, 32),))
    send_slot = draw_send_slot(jax.random.fold_in(seeds[9], 71), 0)
    edge_src = draw_edge_src(jax.random.fold_in(seeds[9], 71), 0)
    w_mesh = bell_draw(seeds[5], (D, D), D ** -0.5, 0.25)
    w_grid = bell_draw(seeds[6], (D, D), D ** -0.5, 0.25)
    w_msg = bell_draw(seeds[7], (D, D), D ** -0.5, 0.25)
    w_out = bell_draw(seeds[8], (D, C), D ** -0.5, 0.25)
    return {"grad_pred": grad_pred, "grid_latent": grid_latent, "mesh_latent": mesh_latent, "send_slot": send_slot, "edge_src": edge_src, "w_mesh": w_mesh, "w_grid": w_grid, "w_msg": w_msg, "w_out": w_out}


def latitude_weight(points, total):
    angle = jnp.pi * ((points.astype(jnp.float32) + 0.5) / total - 0.5)
    return 0.5 * jnp.pi * jnp.cos(angle)

def silu_slope(value):
    sigma = jax.nn.sigmoid(value)
    return sigma * (1.0 + value * (1.0 - sigma))

def reference(grad_pred, grid_latent, mesh_latent, send_slot, edge_src, w_mesh, w_grid, w_msg, w_out):
    points = jnp.arange(GRID, dtype=jnp.int32)
    source_dev = (points // G_DEV).astype(jnp.int32)
    target = (send_slot // CAP).astype(jnp.int32)
    slot_rank = (send_slot % CAP).astype(jnp.int32)
    holder = (target * SLOT_DEV + source_dev * CAP + slot_rank).astype(jnp.int32)
    senders = edge_src[:, holder]
    grid_proj = jnp.dot(grid_latent, w_grid, preferred_element_type=jnp.float32).astype(jnp.bfloat16)
    mesh_proj = jnp.dot(mesh_latent, w_mesh, preferred_element_type=jnp.float32).astype(jnp.bfloat16)
    grid_float = grid_proj.astype(jnp.float32)
    pre_acts = [mesh_proj[senders[corner]].astype(jnp.float32) + grid_float for corner in range(3)]
    act_sum = (jax.nn.silu(pre_acts[0]) + jax.nn.silu(pre_acts[1]) + jax.nn.silu(pre_acts[2])).astype(jnp.bfloat16)
    aggregate = jnp.dot(act_sum, w_msg, preferred_element_type=jnp.float32).astype(jnp.bfloat16)
    weighted = (latitude_weight(points, GRID)[None, :] * grad_pred.astype(jnp.float32)).astype(jnp.bfloat16)
    raw_out = jnp.dot(aggregate.T, weighted.T, preferred_element_type=jnp.float32)
    agg_grad = jnp.dot(weighted.T, w_out.T, preferred_element_type=jnp.float32).astype(jnp.bfloat16)
    raw_msg = jnp.dot(act_sum.T, agg_grad, preferred_element_type=jnp.float32)
    act_grad = jnp.dot(agg_grad, w_msg.T, preferred_element_type=jnp.float32)
    pre_grads = [(act_grad * silu_slope(pre)).astype(jnp.bfloat16) for pre in pre_acts]
    grid_proj_grad = (pre_grads[0].astype(jnp.float32) + pre_grads[1].astype(jnp.float32) + pre_grads[2].astype(jnp.float32)).astype(jnp.bfloat16)
    raw_grid = jnp.dot(grid_latent.T, grid_proj_grad, preferred_element_type=jnp.float32)
    node_total = jnp.zeros((MESH, D), jnp.float32)
    for corner in range(3):
        node_total = node_total.at[senders[corner]].add(pre_grads[corner].astype(jnp.float32))
    mesh_proj_grad = node_total.astype(jnp.bfloat16)
    mesh_grad = jnp.dot(mesh_proj_grad, w_mesh.T, preferred_element_type=jnp.float32).astype(jnp.bfloat16)
    raw_mesh = jnp.dot(mesh_latent.T, mesh_proj_grad, preferred_element_type=jnp.float32)
    grad_scale = 1.0 / math.sqrt(3.0 * GRID)
    return (mesh_grad, raw_mesh * grad_scale, raw_grid * grad_scale, raw_msg * grad_scale, raw_out * grad_scale)
```

```python
import functools
import math

import jax
import jax.numpy as jnp
from jax import lax
from jax.experimental import pallas as pl
from jax.experimental.pallas import tpu as pltpu
from jax.sharding import PartitionSpec as P

HALVES = 2
LANES = 128
TILE = 16


def latitude_weight(points, total):
    angle = jnp.pi * ((points.astype(jnp.float32) + 0.5) / total - 0.5)
    return 0.5 * jnp.pi * jnp.cos(angle)


def contract_rows(left, right):
    return lax.dot_general(
        left, right, (((0,), (0,)), ((), ())), preferred_element_type=jnp.float32
    )


def times_transpose(left, right):
    return lax.dot_general(
        left, right, (((1,), (1,)), ((), ())), preferred_element_type=jnp.float32
    )


def times(left, right):
    return jnp.dot(left, right, preferred_element_type=jnp.float32)


def round_up(value, multiple):
    return -(-value // multiple) * multiple


def remote(src, dst, send_sem, recv_sem, band, sub):
    return pltpu.make_async_remote_copy(
        src_ref=src,
        dst_ref=dst,
        send_sem=send_sem,
        recv_sem=recv_sem,
        device_id=(band, sub),
        device_id_type=pl.DeviceIdType.MESH,
    )


def greet(band, sub):
    pl.semaphore_signal(
        pltpu.get_barrier_semaphore(),
        inc=1,
        device_id=(band, sub),
        device_id_type=pl.DeviceIdType.MESH,
    )


def edge_kernel(
    bands,
    subs,
    capacity,
    slot_ref,
    latent_ref,
    weighted_ref,
    block_ref,
    edge_ref,
    w_mesh_ref,
    w_grid_ref,
    w_msg_ref,
    w_out_ref,
    node_ref,
    parts_ref,
    rows_out,
    grads_out,
    rows_in,
    grads_in,
    table,
    proj,
    edge_in,
    index_cols,
    act_weight,
    hot,
    pre,
    grid_part,
    act_grad,
    act_sum,
    pre_grad,
    grid_grad,
    node_acc,
    grid_acc,
    out_acc,
    rows_send,
    rows_recv,
    grads_send,
    grads_recv,
    half_send,
    pair_send,
    twin_send,
    table_recv,
    edge_send,
    edge_recv,
):
    lows = bands // HALVES
    pairs = subs // 2
    padded = rows_out.shape[2]
    used = subs * capacity
    block_rows, width = block_ref.shape
    patch = subs * block_rows
    points = latent_ref.shape[0]
    band, sub = lax.axis_index("band"), lax.axis_index("sub")
    half, low = band // lows, band % lows
    pair, parity = sub // 2, sub % 2
    twin = 2 * pair + 1 - parity
    group = HALVES * subs
    mine = half * subs + sub

    def low_ahead(step):
        return (low // 2 + step // 2) % (lows // 2) * 2 + (low % 2 + step % 2) % 2

    def low_behind(step):
        return (low // 2 + lows // 2 - step // 2) % (lows // 2) * 2 + (low % 2 + step % 2) % 2

    def member(step):
        index = (mine + step) % group
        return index // subs, index % subs

    @pl.loop(1, group)
    def _(step):
        other_half, other_sub = member(step)
        greet(other_half * lows + low, other_sub)

    @pl.loop(1, lows)
    def _(step):
        greet(half * lows + low_ahead(step), sub)

    pl.semaphore_wait(pltpu.get_barrier_semaphore(), group - 1 + lows - 1)

    def half_copy(source, target):
        return remote(
            block_ref,
            table.at[source, sub],
            half_send.at[target],
            table_recv.at[source, sub],
            target * lows + low,
            sub,
        )

    def pair_copy(src, source_half, source, target):
        place = 2 * source + parity
        return remote(
            src,
            table.at[source_half, place],
            pair_send.at[source_half, target],
            table_recv.at[source_half, place],
            band,
            2 * target + parity,
        )

    def twin_copy(src, source_half, source):
        return remote(
            src,
            table.at[source_half, source],
            twin_send.at[source_half, source // 2],
            table_recv.at[source_half, source],
            band,
            twin,
        )

    def edge_copy(from_half, from_sub, to_half, to_sub):
        return remote(
            edge_ref.at[to_half, to_sub],
            edge_in.at[from_half, from_sub],
            edge_send.at[to_half, to_sub],
            edge_recv.at[from_half, from_sub],
            to_half * lows + low,
            to_sub,
        )

    for step in range(1, HALVES):
        half_copy(half, (half + step) % HALVES).start()
    for step in range(1, pairs):
        pair_copy(block_ref, half, pair, (pair + step) % pairs).start()
    twin_copy(block_ref, half, sub).start()

    @pl.loop(1, group)
    def _(step):
        other_half, other_sub = member(step)
        edge_copy(half, sub, other_half, other_sub).start()

    def spread(target, rows, grads):
        for part in range(HALVES):
            places = lax.broadcasted_iota(jnp.int32, (padded, points), 0)
            places = places + (target * HALVES + part) * padded
            one_hot = jnp.where(places == slot_ref[...], 1.0, 0.0).astype(jnp.bfloat16)
            rows[part] = times(one_hot, latent_ref[...]).astype(jnp.bfloat16)
            grads[part] = times_transpose(one_hot, weighted_ref[...]).astype(jnp.bfloat16)

    def rows_copy(source, target):
        return remote(
            rows_out.at[target],
            rows_in.at[source],
            rows_send.at[target],
            rows_recv.at[source],
            half * lows + target,
            sub,
        )

    def grads_copy(source, target):
        return remote(
            grads_out.at[target],
            grads_in.at[source],
            grads_send.at[target],
            grads_recv.at[source],
            half * lows + target,
            sub,
        )

    @pl.loop(1, lows)
    def _(step):
        target = low_ahead(step)
        spread(target, rows_out.at[target], grads_out.at[target])
        rows_copy(low, target).start()
        grads_copy(low, target).start()

    spread(low, rows_in.at[low], grads_in.at[low])

    table[half, sub] = block_ref[...]
    edge_in[half, sub] = edge_ref[half, sub]
    act_weight[...] = lax.dot_general(
        w_out_ref[...], w_msg_ref[...], (((0,), (1,)), ((), ())), preferred_element_type=jnp.float32
    ).astype(jnp.bfloat16)
    node_acc[...] = jnp.zeros_like(node_acc)
    grid_acc[...] = jnp.zeros_like(grid_acc)
    out_acc[...] = jnp.zeros_like(out_acc)

    def arrived(source_half, source):
        return remote(
            block_ref,
            table.at[source_half, source],
            twin_send.at[0, 0],
            table_recv.at[source_half, source],
            band,
            twin,
        ).wait_recv

    def project(source_half, source):
        rows = pl.ds(pl.multiple_of(source * block_rows, block_rows), block_rows)
        proj[source_half, rows] = times(table[source_half, source], w_mesh_ref[...]).astype(
            jnp.bfloat16
        )

    project(half, sub)
    for step in range(1, pairs):
        source = 2 * ((pair + step) % pairs) + parity
        arrived(half, source)()
        twin_copy(table.at[half, source], half, source).start()
        project(half, source)
    for step in range(1, HALVES):
        source_half = (half + step) % HALVES
        arrived(source_half, sub)()
        place = table.at[source_half, sub]
        twin_copy(place, source_half, sub).start()
        for other in range(1, pairs):
            pair_copy(place, source_half, pair, (pair + other) % pairs).start()
        project(source_half, sub)
    for source_pair in range(pairs):
        source = 2 * source_pair + 1 - parity
        arrived(half, source)()
        project(half, source)
    for step in range(1, HALVES):
        source_half = (half + step) % HALVES
        for other in range(1, pairs):
            source = 2 * ((pair + other) % pairs) + parity
            arrived(source_half, source)()
            twin_copy(table.at[source_half, source], source_half, source).start()
            project(source_half, source)
        for source_pair in range(pairs):
            source = 2 * source_pair + 1 - parity
            arrived(source_half, source)()
            project(source_half, source)

    @pl.loop(1, group)
    def _(step):
        other_half, other_sub = member(step)
        edge_copy(other_half, other_sub, half, sub).wait_recv()

    lanes = index_cols.shape[2]
    count = edge_ref.shape[2]
    for part in range(HALVES):
        total = jnp.zeros((count, lanes), jnp.int32)
        for source in range(subs):
            piece = edge_in[part, source]
            if lanes > LANES:
                piece = jnp.concatenate(
                    [piece, jnp.zeros((count, lanes - LANES), jnp.int32)], axis=1
                )
            if source:
                piece = pltpu.roll(piece, source * capacity, 1)
            total = total + piece
        if count < LANES:
            total = jnp.concatenate([total, jnp.zeros((LANES - count, lanes), jnp.int32)], axis=0)
        flipped = total.T
        for source in range(lows):
            moved = pltpu.roll(flipped, LANES - 3 * source, 1) if source else flipped
            index_cols[source, part] = moved

    def process(source):
        for part in range(HALVES):
            for corner in range(3):
                column = index_cols[source, part, 0:padded, corner : corner + 1]
                nodes = lax.broadcasted_iota(jnp.int32, (padded, patch), 1)
                hot[corner * padded : (corner + 1) * padded, :] = jnp.where(
                    nodes == column, 1.0, 0.0
                ).astype(jnp.bfloat16)
            pre[...] = times(hot[...], proj[part])
            grid_part[...] = times(rows_in[source, part], w_grid_ref[...]).astype(jnp.bfloat16)
            act_grad[...] = times(grads_in[source, part], act_weight[...])

            @pl.loop(0, padded // TILE)
            def _(tile):
                start = pl.multiple_of(tile * TILE, TILE)
                rows = pl.ds(start, TILE)
                base = grid_part[rows].astype(jnp.float32)
                upper = act_grad[rows]
                acts, grads = None, None
                for corner in range(3):
                    place = pl.ds(pl.multiple_of(corner * padded + start, TILE), TILE)
                    value = pre[place] + base
                    sigma = 0.5 * jnp.tanh(0.5 * value) + 0.5
                    act = value * sigma
                    grad = (upper * (sigma + act * (1.0 - sigma))).astype(jnp.bfloat16)
                    pre_grad[place] = grad
                    grad = grad.astype(jnp.float32)
                    acts = act if acts is None else acts + act
                    grads = grad if grads is None else grads + grad
                act_sum[rows] = acts.astype(jnp.bfloat16)
                grid_grad[rows] = grads.astype(jnp.bfloat16)

            out_acc[...] += contract_rows(act_sum[...], grads_in[source, part])
            grid_acc[...] += contract_rows(rows_in[source, part], grid_grad[...])
            node_acc[part] += contract_rows(hot[...], pre_grad[...])

    @pl.loop(0, lows)
    def _(step):
        source = low_behind(step)

        @pl.when(step > 0)
        def _():
            rows_copy(source, source).wait_recv()
            grads_copy(source, source).wait_recv()

        process(source)

    mesh_total = None
    for part in range(HALVES):
        for source in range(subs):
            rows = pl.ds(source * block_rows, block_rows)
            value = node_acc[part, rows].astype(jnp.bfloat16)
            node_ref[part, source] = value
            term = contract_rows(table[part, source], value)
            mesh_total = term if mesh_total is None else mesh_total + term
    parts_ref[:, 0:width] = mesh_total.astype(jnp.bfloat16)
    parts_ref[:, width : 2 * width] = grid_acc[...].astype(jnp.bfloat16)
    parts_ref[:, 2 * width :] = out_acc[...].astype(jnp.bfloat16)

    @pl.loop(1, lows)
    def _(step):
        target = low_ahead(step)
        rows_copy(low, target).wait_send()
        grads_copy(low, target).wait_send()

    for step in range(1, HALVES):
        half_copy(half, (half + step) % HALVES).wait_send()
    for source_half in range(HALVES):
        for step in range(1, pairs):
            pair_copy(block_ref, source_half, pair, (pair + step) % pairs).wait_send()
        for source_pair in range(pairs):
            twin_copy(block_ref, source_half, 2 * source_pair + parity).wait_send()

    @pl.loop(1, group)
    def _(step):
        other_half, other_sub = member(step)
        edge_copy(half, sub, other_half, other_sub).wait_send()


def edge_pass(slots, latent, weighted, block, edges, w_mesh, w_grid, w_msg, w_out, capacity):
    bands, subs = lax.axis_size("band"), lax.axis_size("sub")
    lows, pairs = bands // HALVES, subs // 2
    padded = round_up(subs * capacity, TILE)
    block_rows, width = block.shape
    patch = subs * block_rows
    columns = weighted.shape[0]
    lanes = round_up(padded, LANES)
    vmem = pl.BlockSpec(memory_space=pltpu.VMEM)
    dma = pltpu.SemaphoreType.DMA
    half, full = jnp.bfloat16, jnp.float32
    return pl.pallas_call(
        functools.partial(edge_kernel, bands, subs, capacity),
        out_shape=(
            jax.ShapeDtypeStruct((HALVES, subs, block_rows, width), half),
            jax.ShapeDtypeStruct((width, 2 * width + columns), half),
        ),
        in_specs=[vmem] * 9,
        out_specs=(vmem, vmem),
        scratch_shapes=[
            pltpu.VMEM((lows, HALVES, padded, width), half),
            pltpu.VMEM((lows, HALVES, padded, columns), half),
            pltpu.VMEM((lows, HALVES, padded, width), half),
            pltpu.VMEM((lows, HALVES, padded, columns), half),
            pltpu.VMEM((HALVES, subs, block_rows, width), half),
            pltpu.VMEM((HALVES, patch, width), half),
            pltpu.VMEM(edges.shape, jnp.int32),
            pltpu.VMEM((lows, HALVES, lanes, LANES), jnp.int32),
            pltpu.VMEM((columns, width), half),
            pltpu.VMEM((3 * padded, patch), half),
            pltpu.VMEM((3 * padded, width), full),
            pltpu.VMEM((padded, width), half),
            pltpu.VMEM((padded, width), full),
            pltpu.VMEM((padded, width), half),
            pltpu.VMEM((3 * padded, width), half),
            pltpu.VMEM((padded, width), half),
            pltpu.VMEM((HALVES, patch, width), full),
            pltpu.VMEM((width, width), full),
            pltpu.VMEM((width, columns), full),
        ]
        + [dma((lows,))] * 4
        + [
            dma((HALVES,)),
            dma((HALVES, pairs)),
            dma((HALVES, pairs)),
            dma((HALVES, subs)),
            dma((HALVES, subs)),
            dma((HALVES, subs)),
        ],
        compiler_params=pltpu.CompilerParams(
            collective_id=1, has_side_effects=True, vmem_limit_bytes=64000000
        ),
    )(slots, latent, weighted, block, edges, w_mesh, w_grid, w_msg, w_out)


def reduce_kernel(
    subs,
    parts_ref,
    nodes_ref,
    total_ref,
    node_ref,
    half_in,
    half_sum,
    group_in,
    node_in,
    node_sum,
    node_last,
    node_half,
    node_far,
    half_sem,
    group_send,
    group_recv,
    own_send,
    own_recv,
    pass_send,
    pass_recv,
    node_send,
    node_recv,
    last_send,
    last_recv,
    far_send,
    far_recv,
):
    devices = parts_ref.shape[0]
    groups = devices // 2
    sub_groups = subs // 2
    lows = devices // subs // HALVES
    band, sub = lax.axis_index("band"), lax.axis_index("sub")
    me = band * subs + sub
    own_half, low = band // lows, band % lows
    parity, group = me % 2, me // 2
    other = 1 - parity
    partner = me + 1 - 2 * parity
    own_pair = sub // 2

    def to_device(src, dst, send_sem, recv_sem, device):
        return remote(src, dst, send_sem, recv_sem, device // subs, device % subs)

    def member(index):
        return 2 * index + parity

    def ahead(step):
        return (group + step) % groups

    def behind(step):
        return (group + groups - step) % groups

    greet(partner // subs, partner % subs)

    @pl.loop(1, groups)
    def _(step):
        device = member(ahead(step))
        greet(device // subs, device % subs)

    pl.semaphore_wait(pltpu.get_barrier_semaphore(), groups)

    node_copies = [
        to_device(
            nodes_ref.at[part, 2 * pair + other],
            node_in.at[part, pair],
            node_send.at[part, pair],
            node_recv.at[part, pair],
            partner,
        )
        for part in range(HALVES)
        for pair in range(sub_groups)
    ]
    for copy in node_copies:
        copy.start()
    half_copy = to_device(
        parts_ref.at[pl.ds(other * groups, groups)], half_in, half_sem.at[0], half_sem.at[1], partner
    )
    half_copy.start()
    for copy in node_copies:
        copy.wait()

    def last_copy(part, source, target):
        return to_device(
            node_sum.at[part, target],
            node_last.at[part, source],
            last_send.at[part, target],
            last_recv.at[part, source],
            band * subs + 2 * target + parity,
        )

    def add_node(part, pair):
        return nodes_ref[part, 2 * pair + parity].astype(jnp.float32) + node_in[part, pair].astype(
            jnp.float32
        )

    for turn in range(HALVES):
        part = (own_half + 1 + turn) % HALVES
        for step in range(1, sub_groups):
            target = (own_pair + step) % sub_groups
            node_sum[part, target] = add_node(part, target).astype(node_sum.dtype)
            last_copy(part, own_pair, target).start()

    half_copy.wait()

    def add_half(index):
        return parts_ref[parity * groups + index].astype(jnp.float32) + half_in[index].astype(
            jnp.float32
        )

    def group_copy(source, target):
        return to_device(
            half_sum.at[target],
            group_in.at[source],
            group_send.at[target],
            group_recv.at[source],
            member(target),
        )

    @pl.loop(1, groups)
    def _(step):
        target = ahead(step)
        half_sum[target] = add_half(target).astype(half_sum.dtype)
        group_copy(group, target).start()

    def far_copy(source, target):
        return to_device(
            node_half.at[target],
            node_far.at[source],
            far_send.at[target],
            far_recv.at[source],
            (target * lows + low) * subs + sub,
        )

    def gather_node(part):
        running = add_node(part, own_pair)
        for step in range(1, sub_groups):
            source = (own_pair + sub_groups - step) % sub_groups
            last_copy(part, source, source).wait_recv()
            running = running + node_last[part, source].astype(jnp.float32)
        return running

    for step in range(1, HALVES):
        target = (own_half + step) % HALVES
        node_half[target] = gather_node(target).astype(node_half.dtype)
        far_copy(own_half, target).start()

    def take(step, running):
        source = behind(step)
        group_copy(source, source).wait_recv()
        return running + group_in[source].astype(jnp.float32)

    mine = parity * groups + group
    total_ref[mine] = lax.fori_loop(1, groups, take, add_half(group)).astype(total_ref.dtype)

    def own_copy(source, target):
        place = total_ref.at[parity * groups + source]
        return to_device(place, place, own_send.at[target], own_recv.at[source], member(target))

    def pass_copy(source, half):
        place = total_ref.at[half * groups + source]
        return to_device(place, place, pass_send.at[source], pass_recv.at[source], partner)

    @pl.loop(1, groups)
    def _(step):
        own_copy(group, ahead(step)).start()

    pass_copy(group, parity).start()

    running = gather_node(own_half)
    for step in range(1, HALVES):
        source = (own_half + HALVES - step) % HALVES
        far_copy(source, source).wait_recv()
        running = running + node_far[source].astype(jnp.float32)
    node_ref[...] = running.astype(node_ref.dtype)

    @pl.loop(1, groups)
    def _(step):
        source = behind(step)
        own_copy(source, source).wait_recv()
        pass_copy(source, parity).start()

    @pl.loop(0, groups)
    def _(step):
        source = ahead(step)
        pass_copy(source, other).wait_recv()
        pass_copy(source, parity).wait_send()

    @pl.loop(1, groups)
    def _(step):
        target = ahead(step)
        group_copy(group, target).wait_send()
        own_copy(group, target).wait_send()

    for part in range(HALVES):
        for step in range(1, sub_groups):
            last_copy(part, own_pair, (own_pair + step) % sub_groups).wait_send()
    for step in range(1, HALVES):
        far_copy(own_half, (own_half + step) % HALVES).wait_send()


def reduce_all(parts, nodes):
    devices, rows, columns = parts.shape
    _, subs, node_rows, width = nodes.shape
    groups, sub_groups = devices // 2, subs // 2
    vmem = pl.BlockSpec(memory_space=pltpu.VMEM)
    dma = pltpu.SemaphoreType.DMA
    return pl.pallas_call(
        functools.partial(reduce_kernel, subs),
        out_shape=(
            jax.ShapeDtypeStruct(parts.shape, parts.dtype),
            jax.ShapeDtypeStruct((node_rows, width), nodes.dtype),
        ),
        in_specs=[vmem, vmem],
        out_specs=(vmem, vmem),
        scratch_shapes=[pltpu.VMEM((groups, rows, columns), parts.dtype)] * 3
        + [pltpu.VMEM((HALVES, sub_groups, node_rows, width), nodes.dtype)] * 3
        + [pltpu.VMEM((HALVES, node_rows, width), nodes.dtype)] * 2
        + [dma((2,))]
        + [dma((groups,))] * 6
        + [dma((HALVES, sub_groups))] * 4
        + [dma((HALVES,))] * 2,
        compiler_params=pltpu.CompilerParams(collective_id=0, has_side_effects=True),
    )(parts, nodes)


def shards(grad_pred, grid_latent, mesh_latent, send_slot, edge_src, w_mesh, w_grid, w_msg, w_out):
    both = ("band", "sub")
    grid_rows, width = grid_latent.shape
    channels = grad_pred.shape[0]
    bands, subs = lax.axis_size("band"), lax.axis_size("sub")
    devices = bands * subs
    lows = bands // HALVES
    block_rows = mesh_latent.shape[0]
    capacity = 3 * grid_rows // devices
    padded = round_up(subs * capacity, TILE)
    total_points = grid_rows * devices
    own_index = lax.axis_index(both)
    points = own_index * grid_rows + jnp.arange(grid_rows, dtype=jnp.int32)
    weighted = (
        latitude_weight(points, total_points)[None, :] * grad_pred.astype(jnp.float32)
    ).astype(jnp.bfloat16)
    padding = -channels % LANES
    weighted = jnp.pad(weighted, ((0, padding), (0, 0)))
    w_out = jnp.pad(w_out, ((0, 0), (0, padding)))
    holder, rank = send_slot // capacity, send_slot % capacity
    holder_band, holder_sub = holder // subs, holder % subs
    holder_half, holder_low = holder_band // lows, holder_band % lows
    slots = (holder_low * HALVES + holder_half) * padded + holder_sub * capacity + rank
    local = edge_src - lax.axis_index("band") * (subs * block_rows)
    local = local.reshape(3, HALVES, lows, subs, capacity).transpose(1, 3, 2, 0, 4)
    local = local.reshape(HALVES, subs, 3 * lows, capacity)
    local = jnp.pad(local, ((0, 0), (0, 0), (0, -3 * lows % 8), (0, LANES - capacity)))
    nodes, parts = edge_pass(
        slots[None, :],
        grid_latent,
        weighted,
        mesh_latent,
        local,
        w_mesh,
        w_grid,
        w_msg,
        w_out,
        capacity,
    )
    totals, mesh_proj_grad = reduce_all(
        parts.reshape(devices, width // devices, parts.shape[1]), nodes
    )
    totals = totals.reshape(parts.shape)
    mesh_grad = times_transpose(mesh_proj_grad, w_mesh).astype(jnp.bfloat16)
    grad_scale = 1.0 / math.sqrt(3.0 * total_points)
    outer = totals[:, 2 * width :]
    return (
        mesh_grad,
        totals[:, :width].astype(jnp.float32) * grad_scale,
        totals[:, width : 2 * width].astype(jnp.float32) * grad_scale,
        times_transpose(outer, w_out) * grad_scale,
        contract_rows(w_msg, outer[:, :channels]) * grad_scale,
    )


def solution(mesh):
    placed = (
        P(None, ("band", "sub")),
        P(("band", "sub"), None),
        P(("band", "sub"), None),
        P(("band", "sub")),
        P(None, ("band", "sub")),
        P(),
        P(),
        P(),
        P(),
    )
    return jax.shard_map(
        shards,
        mesh=mesh,
        in_specs=placed,
        out_specs=(P(("band", "sub"), None), P(), P(), P(), P()),
        check_vma=False,
    )
```

```python
import functools
import math

import jax
import jax.numpy as jnp
from jax import lax
from jax.experimental import pallas as pl
from jax.experimental.pallas import tpu as pltpu
from jax.sharding import PartitionSpec as P

HALVES = 2
LANES = 128
TILE = 16


def latitude_weight(points, total):
    angle = jnp.pi * ((points.astype(jnp.float32) + 0.5) / total - 0.5)
    return 0.5 * jnp.pi * jnp.cos(angle)


def contract_rows(left, right):
    return lax.dot_general(
        left, right, (((0,), (0,)), ((), ())), preferred_element_type=jnp.float32
    )


def times_transpose(left, right):
    return lax.dot_general(
        left, right, (((1,), (1,)), ((), ())), preferred_element_type=jnp.float32
    )


def times(left, right):
    return jnp.dot(left, right, preferred_element_type=jnp.float32)


def round_up(value, multiple):
    return -(-value // multiple) * multiple


def remote(src, dst, send_sem, recv_sem, band, sub):
    return pltpu.make_async_remote_copy(
        src_ref=src,
        dst_ref=dst,
        send_sem=send_sem,
        recv_sem=recv_sem,
        device_id=(band, sub),
        device_id_type=pl.DeviceIdType.MESH,
    )


def greet(band, sub):
    pl.semaphore_signal(
        pltpu.get_barrier_semaphore(),
        inc=1,
        device_id=(band, sub),
        device_id_type=pl.DeviceIdType.MESH,
    )


def edge_kernel(
    bands,
    subs,
    capacity,
    slot_ref,
    latent_ref,
    weighted_ref,
    block_ref,
    edge_ref,
    w_mesh_ref,
    w_grid_ref,
    w_msg_ref,
    w_out_ref,
    node_ref,
    outer_ref,
    inner_ref,
    rows_out,
    grads_out,
    rows_in,
    grads_in,
    table,
    proj,
    edge_in,
    index_cols,
    act_weight,
    hot,
    pre,
    grid_part,
    act_grad,
    act_sum,
    pre_grad,
    grid_grad,
    node_acc,
    grid_acc,
    out_acc,
    node_out,
    node_in,
    node_sum,
    node_last,
    node_half,
    node_far,
    outer_parts,
    outer_in,
    outer_near,
    outer_line,
    inner_parts,
    inner_in,
    inner_near,
    inner_line,
    rows_send,
    rows_recv,
    grads_send,
    grads_recv,
    half_send,
    pair_send,
    twin_send,
    table_recv,
    edge_send,
    edge_recv,
    node_send,
    node_recv,
    last_send,
    last_recv,
    far_send,
    far_recv,
    swap_send,
    swap_recv,
    near_send,
    near_recv,
    line_send,
    line_recv,
    back_send,
    back_recv,
    wide_send,
    wide_recv,
    pass_send,
    pass_recv,
):
    lows = bands // HALVES
    pairs = subs // 2
    nears = 2 * pairs
    lines = bands // 2
    padded = rows_out.shape[2]
    block_rows, width = block_ref.shape
    patch = subs * block_rows
    points = latent_ref.shape[0]
    band, sub = lax.axis_index("band"), lax.axis_index("sub")
    half, low = band // lows, band % lows
    pair, parity = sub // 2, sub % 2
    other = 1 - parity
    twin = 2 * pair + other
    group = HALVES * subs
    mine = half * subs + sub
    near, line = (band % 2) * pairs + pair, band // 2

    def low_ahead(step):
        return (low // 2 + step // 2) % (lows // 2) * 2 + (low % 2 + step % 2) % 2

    def low_behind(step):
        return (low // 2 + lows // 2 - step // 2) % (lows // 2) * 2 + (low % 2 + step % 2) % 2

    def member(step):
        index = (mine + step) % group
        return index // subs, index % subs

    def near_device(index):
        return line * 2 + index // pairs, 2 * (index % pairs) + parity

    def line_device(index):
        return index * 2 + band % 2, sub

    @pl.loop(1, group)
    def _(step):
        other_half, other_sub = member(step)
        greet(other_half * lows + low, other_sub)

    @pl.loop(1, lows)
    def _(step):
        greet(half * lows + low_ahead(step), sub)

    @pl.loop(1, nears)
    def _(step):
        greet(*near_device((near + step) % nears))

    @pl.loop(1, lines)
    def _(step):
        greet(*line_device((line + step) % lines))

    pl.semaphore_wait(
        pltpu.get_barrier_semaphore(), group - 1 + lows - 1 + nears - 1 + lines - 1
    )

    def half_copy(source, target):
        return remote(
            block_ref,
            table.at[source, sub],
            half_send.at[target],
            table_recv.at[source, sub],
            target * lows + low,
            sub,
        )

    def pair_copy(src, source_half, source, target):
        place = 2 * source + parity
        return remote(
            src,
            table.at[source_half, place],
            pair_send.at[source_half, target],
            table_recv.at[source_half, place],
            band,
            2 * target + parity,
        )

    def twin_copy(src, source_half, source):
        return remote(
            src,
            table.at[source_half, source],
            twin_send.at[source_half, source // 2],
            table_recv.at[source_half, source],
            band,
            twin,
        )

    def edge_copy(from_half, from_sub, to_half, to_sub):
        return remote(
            edge_ref.at[to_half, to_sub],
            edge_in.at[from_half, from_sub],
            edge_send.at[to_half, to_sub],
            edge_recv.at[from_half, from_sub],
            to_half * lows + low,
            to_sub,
        )

    for step in range(1, pairs):
        pair_copy(block_ref, half, pair, (pair + step) % pairs).start()
    twin_copy(block_ref, half, sub).start()

    @pl.loop(1, group)
    def _(step):
        other_half, other_sub = member(step)
        edge_copy(half, sub, other_half, other_sub).start()

    for step in range(1, HALVES):
        half_copy(half, (half + step) % HALVES).start()

    def spread(target, part, rows, grads):
        places = lax.broadcasted_iota(jnp.int32, (padded, points), 0)
        places = places + (target * HALVES + part) * padded
        one_hot = jnp.where(places == slot_ref[...], 1.0, 0.0).astype(jnp.bfloat16)
        rows[target, part] = times(one_hot, latent_ref[...]).astype(jnp.bfloat16)
        grads[target, part] = times_transpose(one_hot, weighted_ref[...]).astype(jnp.bfloat16)

    def point_copies(source, target, part):
        return (
            remote(
                rows_out.at[target, part],
                rows_in.at[source, part],
                rows_send.at[target, part],
                rows_recv.at[source, part],
                half * lows + target,
                sub,
            ),
            remote(
                grads_out.at[target, part],
                grads_in.at[source, part],
                grads_send.at[target, part],
                grads_recv.at[source, part],
                half * lows + target,
                sub,
            ),
        )

    def split(count):
        return (half + count // lows) % HALVES, count % lows

    @pl.loop(0, HALVES * lows)
    def _(count):
        part, step = split(count)

        @pl.when(step > 0)
        def _():
            target = low_ahead(step)
            spread(target, part, rows_out, grads_out)
            for copy in point_copies(low, target, part):
                copy.start()

    for part in range(HALVES):
        spread(low, part, rows_in, grads_in)

    table[half, sub] = block_ref[...]
    edge_in[half, sub] = edge_ref[half, sub]
    act_weight[...] = lax.dot_general(
        w_out_ref[...], w_msg_ref[...], (((0,), (1,)), ((), ())), preferred_element_type=jnp.float32
    ).astype(jnp.bfloat16)
    node_acc[...] = jnp.zeros_like(node_acc)
    grid_acc[...] = jnp.zeros_like(grid_acc)
    out_acc[...] = jnp.zeros_like(out_acc)

    def arrived(source_half, source):
        remote(
            block_ref,
            table.at[source_half, source],
            twin_send.at[0, 0],
            table_recv.at[source_half, source],
            band,
            twin,
        ).wait_recv()

    def project(source_half, source):
        rows = pl.ds(pl.multiple_of(source * block_rows, block_rows), block_rows)
        proj[source_half, rows] = times(table[source_half, source], w_mesh_ref[...]).astype(
            jnp.bfloat16
        )

    def pass_pairs(source_half):
        for step in range(1, pairs):
            source = 2 * ((pair + step) % pairs) + parity
            arrived(source_half, source)
            twin_copy(table.at[source_half, source], source_half, source).start()

    def finish_table(source_half):
        for source_pair in range(pairs):
            arrived(source_half, 2 * source_pair + other)

        @pl.loop(0, subs)
        def _(source):
            project(source_half, source)

    pass_pairs(half)

    @pl.loop(1, group)
    def _(step):
        other_half, other_sub = member(step)
        edge_copy(other_half, other_sub, half, sub).wait_recv()

    lanes = index_cols.shape[2]
    count = edge_ref.shape[2]
    for part in range(HALVES):
        total = jnp.zeros((count, lanes), jnp.int32)
        for source in range(subs):
            piece = edge_in[part, source]
            if lanes > LANES:
                piece = jnp.concatenate(
                    [piece, jnp.zeros((count, lanes - LANES), jnp.int32)], axis=1
                )
            if source:
                piece = pltpu.roll(piece, source * capacity, 1)
            total = total + piece
        if count < LANES:
            total = jnp.concatenate([total, jnp.zeros((LANES - count, lanes), jnp.int32)], axis=0)
        flipped = total.T
        for source in range(lows):
            moved = pltpu.roll(flipped, LANES - 3 * source, 1) if source else flipped
            index_cols[source, part] = moved

    finish_table(half)

    def process(source, part):
        for corner in range(3):
            column = index_cols[source, part, 0:padded, corner : corner + 1]
            nodes = lax.broadcasted_iota(jnp.int32, (padded, patch), 1)
            hot[corner * padded : (corner + 1) * padded, :] = jnp.where(
                nodes == column, 1.0, 0.0
            ).astype(jnp.bfloat16)
        pre[...] = times(hot[...], proj[part])
        grid_part[...] = times(rows_in[source, part], w_grid_ref[...]).astype(jnp.bfloat16)
        act_grad[...] = times(grads_in[source, part], act_weight[...])

        @pl.loop(0, padded // TILE)
        def _(tile):
            start = pl.multiple_of(tile * TILE, TILE)
            rows = pl.ds(start, TILE)
            base = grid_part[rows].astype(jnp.float32)
            upper = act_grad[rows]
            acts, grads = None, None
            for corner in range(3):
                place = pl.ds(pl.multiple_of(corner * padded + start, TILE), TILE)
                value = pre[place] + base
                sigma = 0.5 * jnp.tanh(0.5 * value) + 0.5
                act = value * sigma
                grad = (upper * (sigma + act * (1.0 - sigma))).astype(jnp.bfloat16)
                pre_grad[place] = grad
                grad = grad.astype(jnp.float32)
                acts = act if acts is None else acts + act
                grads = grad if grads is None else grads + grad
            act_sum[rows] = acts.astype(jnp.bfloat16)
            grid_grad[rows] = grads.astype(jnp.bfloat16)

        out_acc[...] += contract_rows(act_sum[...], grads_in[source, part])
        grid_acc[...] += contract_rows(rows_in[source, part], grid_grad[...])
        node_acc[part] += contract_rows(hot[...], pre_grad[...])

    def node_copies(part):
        return [
            remote(
                node_out.at[part, 2 * index + other],
                node_in.at[part, index],
                node_send.at[part, index],
                node_recv.at[part, index],
                band,
                twin,
            )
            for index in range(pairs)
        ]

    def last_copy(part, source, target):
        return remote(
            node_sum.at[part, target],
            node_last.at[part, source],
            last_send.at[part, target],
            last_recv.at[part, source],
            band,
            2 * target + parity,
        )

    def far_copy(source, target):
        return remote(
            node_half.at[target],
            node_far.at[source],
            far_send.at[target],
            far_recv.at[source],
            target * lows + low,
            sub,
        )

    def add_node(part, index):
        return node_out[part, 2 * index + parity].astype(jnp.float32) + node_in[
            part, index
        ].astype(jnp.float32)

    def swap_nodes(part):
        for source in range(subs):
            rows = pl.ds(source * block_rows, block_rows)
            node_out[part, source] = node_acc[part, rows].astype(jnp.bfloat16)
        for copy in node_copies(part):
            copy.start()

    def send_nodes(part):
        for copy in node_copies(part):
            copy.wait()
        for step in range(1, pairs):
            target = (pair + step) % pairs
            node_sum[part, target] = add_node(part, target).astype(jnp.bfloat16)
            last_copy(part, pair, target).start()

    def gather_node(part):
        running = add_node(part, pair)
        for step in range(1, pairs):
            source = (pair + pairs - step) % pairs
            last_copy(part, source, source).wait_recv()
            running = running + node_last[part, source].astype(jnp.float32)
        return running

    @pl.loop(0, HALVES * lows)
    def _(count):
        part, step = split(count)
        source = low_behind(step)

        @pl.when(count == lows // 2)
        def _():
            for turn in range(1, HALVES):
                source_half = (half + turn) % HALVES
                arrived(source_half, sub)
                place = table.at[source_half, sub]
                twin_copy(place, source_half, sub).start()
                for index in range(1, pairs):
                    pair_copy(place, source_half, pair, (pair + index) % pairs).start()

        @pl.when(count == lows - 1)
        def _():
            for turn in range(1, HALVES):
                pass_pairs((half + turn) % HALVES)

        @pl.when(count == lows)
        def _():
            for turn in range(1, HALVES):
                finish_table((half + turn) % HALVES)
            swap_nodes(half)

        @pl.when(count == lows + 1)
        def _():
            send_nodes(half)

        @pl.when(step > 0)
        def _():
            for copy in point_copies(source, source, part):
                copy.wait_recv()

        process(source, part)

    for turn in range(1, HALVES):
        swap_nodes((half + turn) % HALVES)

    chunks = (
        (outer_parts, outer_in, outer_near, outer_line, outer_ref),
        (inner_parts, inner_in, inner_near, inner_line, inner_ref),
    )

    def swap_copy(index):
        parts, arriving = chunks[index][:2]
        return remote(
            parts.at[other], arriving, swap_send.at[index], swap_recv.at[index], band, twin
        )

    def near_copy(index, source, target):
        parts, _, arriving = chunks[index][:3]
        return remote(
            parts.at[parity, target],
            arriving.at[source],
            near_send.at[index, target],
            near_recv.at[index, source],
            *near_device(target),
        )

    def line_copy(index, source, target):
        parts, _, _, arriving = chunks[index][:4]
        return remote(
            parts.at[parity, near, target],
            arriving.at[source],
            line_send.at[index, target],
            line_recv.at[index, source],
            *line_device(target),
        )

    def back_copy(index, source, target):
        place = chunks[index][4].at[parity, near, source]
        return remote(
            place,
            place,
            back_send.at[index, target],
            back_recv.at[index, source],
            *line_device(target),
        )

    def wide_copy(index, source, target):
        place = chunks[index][4].at[parity, source]
        return remote(
            place,
            place,
            wide_send.at[index, target],
            wide_recv.at[index, source],
            *near_device(target),
        )

    def pass_copy(index, source, side):
        place = chunks[index][4].at[side, source]
        return remote(
            place, place, pass_send.at[index, source], pass_recv.at[index, source], band, twin
        )

    rows = outer_parts.shape[3]

    def fill(parts, value, first):
        for device in range(nears * lines * 2):
            place = (device // (nears * lines), device // lines % nears, device % lines)
            piece = value[device * rows : (device + 1) * rows]
            parts[place + (slice(None), slice(first, first + value.shape[1]))] = piece.astype(
                jnp.bfloat16
            )

    fill(outer_parts, grid_acc[...], 0)
    fill(outer_parts, out_acc[...], width)
    swap_copy(0).start()
    mesh_total = None
    for part in range(HALVES):
        for source in range(subs):
            term = contract_rows(table[part, source], node_out[part, source])
            mesh_total = term if mesh_total is None else mesh_total + term
    fill(inner_parts, mesh_total, 0)
    swap_copy(1).start()

    for turn in range(1, HALVES):
        send_nodes((half + turn) % HALVES)

    def add_up(left, right):
        return (left.astype(jnp.float32) + right.astype(jnp.float32)).astype(jnp.bfloat16)

    for index, (parts, arriving, _, _, _) in enumerate(chunks):
        swap_copy(index).wait()

        @pl.loop(1, nears)
        def _(step):
            target = (near + step) % nears
            parts[parity, target] = add_up(parts[parity, target], arriving[target])
            near_copy(index, near, target).start()

    for turn in range(1, HALVES):
        target = (half + turn) % HALVES
        node_half[target] = gather_node(target).astype(jnp.bfloat16)
        far_copy(half, target).start()

    for index, (parts, arriving, close, _, _) in enumerate(chunks):

        def take_near(step, running):
            source = (near + nears - step) % nears
            near_copy(index, source, source).wait_recv()
            return running + close[source].astype(jnp.float32)

        running = parts[parity, near].astype(jnp.float32) + arriving[near].astype(jnp.float32)
        for step in range(1, nears):
            running = take_near(step, running)
        parts[parity, near] = running.astype(jnp.bfloat16)

        @pl.loop(1, lines)
        def _(step):
            line_copy(index, line, (line + step) % lines).start()

    for index, (parts, _, _, arriving, total) in enumerate(chunks):

        def take_line(step, running):
            source = (line + lines - step) % lines
            line_copy(index, source, source).wait_recv()
            return running + arriving[source].astype(jnp.float32)

        running = parts[parity, near, line].astype(jnp.float32)
        running = lax.fori_loop(1, lines, take_line, running)
        total[parity, near, line] = running.astype(jnp.bfloat16)

        @pl.loop(1, lines)
        def _(step):
            back_copy(index, line, (line + step) % lines).start()

    for index in range(2):

        @pl.loop(1, lines)
        def _(step):
            source = (line + lines - step) % lines
            back_copy(index, source, source).wait_recv()

        @pl.loop(1, nears)
        def _(step):
            wide_copy(index, near, (near + step) % nears).start()

        pass_copy(index, near, parity).start()

    running = gather_node(half)
    for turn in range(1, HALVES):
        source = (half + HALVES - turn) % HALVES
        far_copy(source, source).wait_recv()
        running = running + node_far[source].astype(jnp.float32)
    node_ref[...] = times_transpose(running.astype(jnp.bfloat16), w_mesh_ref[...]).astype(
        jnp.bfloat16
    )

    for index in range(2):

        @pl.loop(1, nears)
        def _(step):
            source = (near + nears - step) % nears
            wide_copy(index, source, source).wait_recv()
            pass_copy(index, source, parity).start()

    for index in range(2):

        @pl.loop(0, nears)
        def _(source):
            pass_copy(index, source, other).wait_recv()
            pass_copy(index, source, parity).wait_send()

        @pl.loop(1, nears)
        def _(step):
            near_copy(index, near, (near + step) % nears).wait_send()
            wide_copy(index, near, (near + step) % nears).wait_send()

        @pl.loop(1, lines)
        def _(step):
            line_copy(index, line, (line + step) % lines).wait_send()
            back_copy(index, line, (line + step) % lines).wait_send()

    @pl.loop(0, HALVES * lows)
    def _(count):
        part, step = split(count)

        @pl.when(step > 0)
        def _():
            for copy in point_copies(low, low_ahead(step), part):
                copy.wait_send()

    for step in range(1, HALVES):
        half_copy(half, (half + step) % HALVES).wait_send()
        far_copy(half, (half + step) % HALVES).wait_send()
    for source_half in range(HALVES):
        for step in range(1, pairs):
            pair_copy(block_ref, source_half, pair, (pair + step) % pairs).wait_send()
            last_copy(source_half, pair, (pair + step) % pairs).wait_send()
        for source_pair in range(pairs):
            twin_copy(block_ref, source_half, 2 * source_pair + parity).wait_send()

    @pl.loop(1, group)
    def _(step):
        other_half, other_sub = member(step)
        edge_copy(half, sub, other_half, other_sub).wait_send()


def edge_pass(slots, latent, weighted, block, edges, w_mesh, w_grid, w_msg, w_out, capacity):
    bands, subs = lax.axis_size("band"), lax.axis_size("sub")
    lows, pairs = bands // HALVES, subs // 2
    nears, lines = 2 * pairs, bands // 2
    padded = round_up(subs * capacity, TILE)
    block_rows, width = block.shape
    patch = subs * block_rows
    columns = weighted.shape[0]
    lanes = round_up(padded, LANES)
    rows = width // (2 * nears * lines)
    vmem = pl.BlockSpec(memory_space=pltpu.VMEM)
    dma = pltpu.SemaphoreType.DMA
    half, full = jnp.bfloat16, jnp.float32

    def chunk(size):
        return [
            pltpu.VMEM((2, nears, lines, rows, size), half),
            pltpu.VMEM((nears, lines, rows, size), half),
            pltpu.VMEM((nears, lines, rows, size), half),
            pltpu.VMEM((lines, rows, size), half),
        ]

    return pl.pallas_call(
        functools.partial(edge_kernel, bands, subs, capacity),
        out_shape=(
            jax.ShapeDtypeStruct((block_rows, width), half),
            jax.ShapeDtypeStruct((2, nears, lines, rows, width + columns), half),
            jax.ShapeDtypeStruct((2, nears, lines, rows, width), half),
        ),
        in_specs=[vmem] * 9,
        out_specs=(vmem, vmem, vmem),
        scratch_shapes=[
            pltpu.VMEM((lows, HALVES, padded, width), half),
            pltpu.VMEM((lows, HALVES, padded, columns), half),
            pltpu.VMEM((lows, HALVES, padded, width), half),
            pltpu.VMEM((lows, HALVES, padded, columns), half),
            pltpu.VMEM((HALVES, subs, block_rows, width), half),
            pltpu.VMEM((HALVES, patch, width), half),
            pltpu.VMEM(edges.shape, jnp.int32),
            pltpu.VMEM((lows, HALVES, lanes, LANES), jnp.int32),
            pltpu.VMEM((columns, width), half),
            pltpu.VMEM((3 * padded, patch), half),
            pltpu.VMEM((3 * padded, width), full),
            pltpu.VMEM((padded, width), half),
            pltpu.VMEM((padded, width), full),
            pltpu.VMEM((padded, width), half),
            pltpu.VMEM((3 * padded, width), half),
            pltpu.VMEM((padded, width), half),
            pltpu.VMEM((HALVES, patch, width), full),
            pltpu.VMEM((width, width), full),
            pltpu.VMEM((width, columns), full),
            pltpu.VMEM((HALVES, subs, block_rows, width), half),
        ]
        + [pltpu.VMEM((HALVES, pairs, block_rows, width), half)] * 3
        + [pltpu.VMEM((HALVES, block_rows, width), half)] * 2
        + chunk(width + columns)
        + chunk(width)
        + [dma((lows, HALVES))] * 4
        + [
            dma((HALVES,)),
            dma((HALVES, pairs)),
            dma((HALVES, pairs)),
            dma((HALVES, subs)),
            dma((HALVES, subs)),
            dma((HALVES, subs)),
        ]
        + [dma((HALVES, pairs))] * 4
        + [dma((HALVES,))] * 2
        + [dma((2,))] * 2
        + [dma((2, nears))] * 2
        + [dma((2, lines))] * 4
        + [dma((2, nears))] * 4,
        compiler_params=pltpu.CompilerParams(
            collective_id=0, has_side_effects=True, vmem_limit_bytes=64000000
        ),
    )(slots, latent, weighted, block, edges, w_mesh, w_grid, w_msg, w_out)


def shards(grad_pred, grid_latent, mesh_latent, send_slot, edge_src, w_mesh, w_grid, w_msg, w_out):
    both = ("band", "sub")
    grid_rows, width = grid_latent.shape
    channels = grad_pred.shape[0]
    bands, subs = lax.axis_size("band"), lax.axis_size("sub")
    devices = bands * subs
    lows = bands // HALVES
    block_rows = mesh_latent.shape[0]
    capacity = 3 * grid_rows // devices
    padded = round_up(subs * capacity, TILE)
    total_points = grid_rows * devices
    own_index = lax.axis_index(both)
    points = own_index * grid_rows + jnp.arange(grid_rows, dtype=jnp.int32)
    weighted = (
        latitude_weight(points, total_points)[None, :] * grad_pred.astype(jnp.float32)
    ).astype(jnp.bfloat16)
    padding = -channels % LANES
    weighted = jnp.pad(weighted, ((0, padding), (0, 0)))
    w_out = jnp.pad(w_out, ((0, 0), (0, padding)))
    holder, rank = send_slot // capacity, send_slot % capacity
    holder_band, holder_sub = holder // subs, holder % subs
    holder_half, holder_low = holder_band // lows, holder_band % lows
    slots = (holder_low * HALVES + holder_half) * padded + holder_sub * capacity + rank
    local = edge_src - lax.axis_index("band") * (subs * block_rows)
    local = local.reshape(3, HALVES, lows, subs, capacity).transpose(1, 3, 2, 0, 4)
    local = local.reshape(HALVES, subs, 3 * lows, capacity)
    local = jnp.pad(local, ((0, 0), (0, 0), (0, -3 * lows % 8), (0, LANES - capacity)))
    mesh_grad, outer, inner = edge_pass(
        slots[None, :],
        grid_latent,
        weighted,
        mesh_latent,
        local,
        w_mesh,
        w_grid,
        w_msg,
        w_out,
        capacity,
    )
    grad_scale = 1.0 / math.sqrt(3.0 * total_points)
    outer = outer.reshape(width, outer.shape[-1])
    inner = inner.reshape(width, width)
    channel_part = outer[:, width:]
    return (
        mesh_grad,
        inner.astype(jnp.float32) * grad_scale,
        outer[:, :width].astype(jnp.float32) * grad_scale,
        times_transpose(channel_part, w_out) * grad_scale,
        contract_rows(w_msg, channel_part[:, :channels]) * grad_scale,
    )


def solution(mesh):
    placed = (
        P(None, ("band", "sub")),
        P(("band", "sub"), None),
        P(("band", "sub"), None),
        P(("band", "sub")),
        P(None, ("band", "sub")),
        P(),
        P(),
        P(),
        P(),
    )
    return jax.shard_map(
        shards,
        mesh=mesh,
        in_specs=placed,
        out_specs=(P(("band", "sub"), None), P(), P(), P(), P()),
        check_vma=False,
    )
```

```python
import functools
import math

import jax
import jax.numpy as jnp
from jax import lax
from jax.experimental import pallas as pl
from jax.experimental.pallas import tpu as pltpu
from jax.sharding import PartitionSpec as P

HALVES = 2
LANES = 128
TILE = 16
SPAN = 256


def latitude_weight(points, total):
    angle = jnp.pi * ((points.astype(jnp.float32) + 0.5) / total - 0.5)
    return 0.5 * jnp.pi * jnp.cos(angle)


def contract_rows(left, right):
    return lax.dot_general(
        left, right, (((0,), (0,)), ((), ())), preferred_element_type=jnp.float32
    )


def times_transpose(left, right):
    return lax.dot_general(
        left, right, (((1,), (1,)), ((), ())), preferred_element_type=jnp.float32
    )


def times(left, right):
    return jnp.dot(left, right, preferred_element_type=jnp.float32)


def round_up(value, multiple):
    return -(-value // multiple) * multiple


def remote(src, dst, send_sem, recv_sem, band, sub):
    return pltpu.make_async_remote_copy(
        src_ref=src,
        dst_ref=dst,
        send_sem=send_sem,
        recv_sem=recv_sem,
        device_id=(band, sub),
        device_id_type=pl.DeviceIdType.MESH,
    )


def greet(band, sub):
    pl.semaphore_signal(
        pltpu.get_barrier_semaphore(),
        inc=1,
        device_id=(band, sub),
        device_id_type=pl.DeviceIdType.MESH,
    )


def edge_kernel(
    bands,
    subs,
    capacity,
    slot_ref,
    latent_ref,
    weighted_ref,
    block_ref,
    edge_ref,
    w_mesh_ref,
    w_grid_ref,
    w_msg_ref,
    w_out_ref,
    node_ref,
    outer_ref,
    inner_ref,
    cargo,
    weighted,
    w_out,
    rows_out,
    rows_in,
    table,
    proj,
    edge_in,
    index_cols,
    act_weight,
    hot,
    pre,
    grid_part,
    act_grad,
    act_sum,
    pre_grad,
    grid_grad,
    node_acc,
    grid_acc,
    out_acc,
    node_out,
    node_in,
    node_sum,
    node_last,
    node_half,
    node_far,
    outer_parts,
    outer_in,
    outer_near,
    outer_line,
    inner_parts,
    inner_in,
    inner_near,
    inner_line,
    rows_send,
    rows_recv,
    half_send,
    pair_send,
    twin_send,
    table_recv,
    edge_send,
    edge_recv,
    node_send,
    node_recv,
    last_send,
    last_recv,
    far_send,
    far_recv,
    swap_send,
    swap_recv,
    near_send,
    near_recv,
    line_send,
    line_recv,
    back_send,
    back_recv,
    wide_send,
    wide_recv,
    pass_send,
    pass_recv,
):
    lows = bands // HALVES
    pairs = subs // 2
    nears = 2 * pairs
    lines = bands // 2
    padded = rows_out.shape[2]
    block_rows, width = block_ref.shape
    patch = subs * block_rows
    points = latent_ref.shape[0]
    band, sub = lax.axis_index("band"), lax.axis_index("sub")
    half, low = band // lows, band % lows
    pair, parity = sub // 2, sub % 2
    other = 1 - parity
    twin = 2 * pair + other
    group = HALVES * subs
    mine = half * subs + sub
    near, line = (band % 2) * pairs + pair, band // 2

    def low_ahead(step):
        return (low // 2 + step // 2) % (lows // 2) * 2 + (low % 2 + step % 2) % 2

    def low_behind(step):
        return (low // 2 + lows // 2 - step // 2) % (lows // 2) * 2 + (low % 2 + step % 2) % 2

    def member(step):
        index = (mine + step) % group
        return index // subs, index % subs

    def near_device(index):
        return line * 2 + index // pairs, 2 * (index % pairs) + parity

    def line_device(index):
        return index * 2 + band % 2, sub

    @pl.loop(1, group)
    def _(step):
        other_half, other_sub = member(step)
        greet(other_half * lows + low, other_sub)

    @pl.loop(1, lows)
    def _(step):
        greet(half * lows + low_ahead(step), sub)

    @pl.loop(1, nears)
    def _(step):
        greet(*near_device((near + step) % nears))

    @pl.loop(1, lines)
    def _(step):
        greet(*line_device((line + step) % lines))

    pl.semaphore_wait(
        pltpu.get_barrier_semaphore(), group - 1 + lows - 1 + nears - 1 + lines - 1
    )

    def half_copy(source, target):
        return remote(
            block_ref,
            table.at[source, sub],
            half_send.at[target],
            table_recv.at[source, sub],
            target * lows + low,
            sub,
        )

    def pair_copy(src, source_half, source, target):
        place = 2 * source + parity
        return remote(
            src,
            table.at[source_half, place],
            pair_send.at[source_half, target],
            table_recv.at[source_half, place],
            band,
            2 * target + parity,
        )

    def twin_copy(src, source_half, source):
        return remote(
            src,
            table.at[source_half, source],
            twin_send.at[source_half, source // 2],
            table_recv.at[source_half, source],
            band,
            twin,
        )

    def edge_copy(from_half, from_sub, to_half, to_sub):
        return remote(
            edge_ref.at[to_half, to_sub],
            edge_in.at[from_half, from_sub],
            edge_send.at[to_half, to_sub],
            edge_recv.at[from_half, from_sub],
            to_half * lows + low,
            to_sub,
        )

    for step in range(1, pairs):
        pair_copy(block_ref, half, pair, (pair + step) % pairs).start()
    twin_copy(block_ref, half, sub).start()

    @pl.loop(1, group)
    def _(step):
        other_half, other_sub = member(step)
        edge_copy(half, sub, other_half, other_sub).start()

    for step in range(1, HALVES):
        half_copy(half, (half + step) % HALVES).start()

    channels = weighted_ref.shape[0]
    weighted[...] = jnp.zeros_like(weighted)
    weighted[0:channels, :] = weighted_ref[...]
    cargo[:, 0:width] = latent_ref[...]
    cargo[:, width:] = weighted[...].astype(jnp.float32).T.astype(jnp.bfloat16)

    def spread(target, part, rows):
        places = lax.broadcasted_iota(jnp.int32, (padded, points), 0)
        places = places + (target * HALVES + part) * padded
        one_hot = jnp.where(places == slot_ref[...], 1.0, 0.0).astype(jnp.bfloat16)
        rows[target, part] = times(one_hot, cargo[...]).astype(jnp.bfloat16)

    def point_copy(source, target, part):
        return remote(
            rows_out.at[target, part],
            rows_in.at[source, part],
            rows_send.at[target, part],
            rows_recv.at[source, part],
            half * lows + target,
            sub,
        )

    def split(count):
        block = lows // 2
        turn = (count // block + 1) // 2
        return (half + turn) % HALVES, count - block * turn

    @pl.loop(0, HALVES * lows)
    def _(count):
        part, step = split(count)

        @pl.when(step > 0)
        def _():
            target = low_ahead(step)
            spread(target, part, rows_out)
            point_copy(low, target, part).start()

    for part in range(HALVES):
        spread(low, part, rows_in)

    table[half, sub] = block_ref[...]
    edge_in[half, sub] = edge_ref[half, sub]
    w_out[...] = jnp.zeros_like(w_out)
    w_out[:, 0:channels] = w_out_ref[...]
    act_weight[...] = 0.5 * lax.dot_general(
        w_out[...], w_msg_ref[...], (((0,), (1,)), ((), ())), preferred_element_type=jnp.float32
    ).astype(jnp.bfloat16)
    node_acc[...] = jnp.zeros_like(node_acc)
    grid_acc[...] = jnp.zeros_like(grid_acc)
    out_acc[...] = jnp.zeros_like(out_acc)

    def arrived(source_half, source):
        remote(
            block_ref,
            table.at[source_half, source],
            twin_send.at[0, 0],
            table_recv.at[source_half, source],
            band,
            twin,
        ).wait_recv()

    def project(source_half, source):
        rows = pl.ds(pl.multiple_of(source * block_rows, block_rows), block_rows)
        proj[source_half, rows] = 0.5 * times(
            table[source_half, source], w_mesh_ref[...]
        ).astype(jnp.bfloat16)

    def pass_pairs(source_half):
        for step in range(1, pairs):
            source = 2 * ((pair + step) % pairs) + parity
            arrived(source_half, source)
            twin_copy(table.at[source_half, source], source_half, source).start()

    def finish_table(source_half):
        for source_pair in range(pairs):
            arrived(source_half, 2 * source_pair + other)

        @pl.loop(0, subs)
        def _(source):
            project(source_half, source)

    pass_pairs(half)

    @pl.loop(1, group)
    def _(step):
        other_half, other_sub = member(step)
        edge_copy(other_half, other_sub, half, sub).wait_recv()

    lanes = index_cols.shape[2]
    count = edge_ref.shape[2]
    for part in range(HALVES):
        total = jnp.zeros((count, lanes), jnp.int32)
        for source in range(subs):
            piece = edge_in[part, source]
            if lanes > LANES:
                piece = jnp.concatenate(
                    [piece, jnp.zeros((count, lanes - LANES), jnp.int32)], axis=1
                )
            if source:
                piece = pltpu.roll(piece, source * capacity, 1)
            total = total + piece
        if count < LANES:
            total = jnp.concatenate([total, jnp.zeros((LANES - count, lanes), jnp.int32)], axis=0)
        flipped = total.T
        for source in range(lows):
            moved = pltpu.roll(flipped, LANES - 3 * source, 1) if source else flipped
            index_cols[source, part] = moved

    finish_table(half)

    for turn in range(1, HALVES):
        source_half = (half + turn) % HALVES
        arrived(source_half, sub)
        place = table.at[source_half, sub]
        twin_copy(place, source_half, sub).start()
        for index in range(1, pairs):
            pair_copy(place, source_half, pair, (pair + index) % pairs).start()

    def scatter(count, block):
        part, _ = split(count)
        slot = count % 2
        nodes = slice(block * SPAN, (block + 1) * SPAN)
        node_acc[part, nodes] += contract_rows(hot[slot, :, nodes], pre_grad[slot])

    def process(count, scattered):
        part, step = split(count)
        source = low_behind(step)
        slot = count % 2
        for corner in range(3):
            column = index_cols[source, part, 0:padded, corner : corner + 1]
            nodes = lax.broadcasted_iota(jnp.int32, (padded, patch), 1)
            hot[slot, corner * padded : (corner + 1) * padded, :] = jnp.where(
                nodes == column, 1.0, 0.0
            ).astype(jnp.bfloat16)
        latents = rows_in[source, part, :, 0:width]
        losses = rows_in[source, part, :, width:]
        pre[...] = times(hot[slot], proj[part])
        grid_part[...] = 0.5 * times(latents, w_grid_ref[...]).astype(jnp.bfloat16)
        act_grad[...] = times(losses, act_weight[...])

        def finish(start):
            rows = pl.ds(start, TILE)
            base = grid_part[rows].astype(jnp.float32)
            upper = act_grad[rows]
            acts, grads = None, None
            for corner in range(3):
                place = pl.ds(corner * padded + start, TILE)
                value = pre[place] + base
                tanh = jnp.tanh(value)
                above = 1.0 + tanh
                act = value * above
                grad = upper * (above + act * (1.0 - tanh))
                pre_grad[slot, place] = grad.astype(jnp.bfloat16)
                acts = act if acts is None else acts + act
                grads = grad if grads is None else grads + grad
            act_sum[rows] = acts.astype(jnp.bfloat16)
            grid_grad[rows] = grads.astype(jnp.bfloat16)

        tiles = padded // TILE
        blocks = patch // SPAN
        done = 0
        for tile in range(tiles):
            while scattered and done * tiles < (tile + 1) * blocks:
                scatter(count - 1, done)
                done += 1
            finish(tile * TILE)

        out_acc[...] += contract_rows(act_sum[...], losses)
        grid_acc[...] += contract_rows(latents, grid_grad[...])

    def node_copies(part):
        return [
            remote(
                node_out.at[part, 2 * index + other],
                node_in.at[part, index],
                node_send.at[part, index],
                node_recv.at[part, index],
                band,
                twin,
            )
            for index in range(pairs)
        ]

    def last_copy(part, source, target):
        return remote(
            node_sum.at[part, target],
            node_last.at[part, source],
            last_send.at[part, target],
            last_recv.at[part, source],
            band,
            2 * target + parity,
        )

    def far_copy(source, target):
        return remote(
            node_half.at[target],
            node_far.at[source],
            far_send.at[target],
            far_recv.at[source],
            target * lows + low,
            sub,
        )

    def add_node(part, index):
        return node_out[part, 2 * index + parity].astype(jnp.float32) + node_in[
            part, index
        ].astype(jnp.float32)

    def swap_nodes(part):
        for source in range(subs):
            rows = pl.ds(source * block_rows, block_rows)
            node_out[part, source] = node_acc[part, rows].astype(jnp.bfloat16)
        for copy in node_copies(part):
            copy.start()

    def send_nodes(part):
        for copy in node_copies(part):
            copy.wait()
        for step in range(1, pairs):
            target = (pair + step) % pairs
            node_sum[part, target] = add_node(part, target).astype(jnp.bfloat16)
            last_copy(part, pair, target).start()

    def gather_node(part):
        running = add_node(part, pair)
        for step in range(1, pairs):
            source = (pair + pairs - step) % pairs
            last_copy(part, source, source).wait_recv()
            running = running + node_last[part, source].astype(jnp.float32)
        return running

    process(0, False)

    @pl.loop(1, HALVES * lows)
    def _(count):
        part, step = split(count)
        source = low_behind(step)

        @pl.when(count == lows // 2)
        def _():
            for turn in range(1, HALVES):
                pass_pairs((half + turn) % HALVES)
                finish_table((half + turn) % HALVES)

        @pl.when(count == lows // 2 + lows + 1)
        def _():
            for turn in range(1, HALVES):
                swap_nodes((half + turn) % HALVES)

        @pl.when(step > 0)
        def _():
            point_copy(source, source, part).wait_recv()

        process(count, True)

    chunks = (
        (outer_parts, outer_in, outer_near, outer_line, outer_ref),
        (inner_parts, inner_in, inner_near, inner_line, inner_ref),
    )

    def swap_copy(index):
        parts, arriving = chunks[index][:2]
        return remote(
            parts.at[other], arriving, swap_send.at[index], swap_recv.at[index], band, twin
        )

    def near_copy(index, source, target):
        parts, _, arriving = chunks[index][:3]
        return remote(
            parts.at[parity, target],
            arriving.at[source],
            near_send.at[index, target],
            near_recv.at[index, source],
            *near_device(target),
        )

    def line_copy(index, source, target):
        parts, _, _, arriving = chunks[index][:4]
        return remote(
            parts.at[parity, near, target],
            arriving.at[source],
            line_send.at[index, target],
            line_recv.at[index, source],
            *line_device(target),
        )

    def back_copy(index, source, target):
        place = chunks[index][4].at[parity, near, source]
        return remote(
            place,
            place,
            back_send.at[index, target],
            back_recv.at[index, source],
            *line_device(target),
        )

    def wide_copy(index, source, target):
        place = chunks[index][4].at[parity, source]
        return remote(
            place,
            place,
            wide_send.at[index, target],
            wide_recv.at[index, source],
            *near_device(target),
        )

    def pass_copy(index, source, side):
        place = chunks[index][4].at[side, source]
        return remote(
            place, place, pass_send.at[index, source], pass_recv.at[index, source], band, twin
        )

    rows = outer_parts.shape[3]

    def fill(parts, value, first):
        for device in range(nears * lines * 2):
            place = (device // (nears * lines), device // lines % nears, device % lines)
            piece = value[device * rows : (device + 1) * rows]
            parts[place + (slice(None), slice(first, first + value.shape[1]))] = piece.astype(
                jnp.bfloat16
            )

    fill(outer_parts, grid_acc[...], 0)
    fill(outer_parts, out_acc[...], width)
    swap_copy(0).start()
    for turn in range(1, HALVES):
        send_nodes((half + turn) % HALVES)
    for block in range(patch // SPAN):
        scatter(HALVES * lows - 1, block)
    swap_nodes(half)
    mesh_total = None
    for part in range(HALVES):
        for source in range(subs):
            term = contract_rows(table[part, source], node_out[part, source])
            mesh_total = term if mesh_total is None else mesh_total + term
    fill(inner_parts, mesh_total, 0)
    swap_copy(1).start()

    def add_up(left, right):
        return (left.astype(jnp.float32) + right.astype(jnp.float32)).astype(jnp.bfloat16)

    def start_near(index):
        parts, arriving = chunks[index][:2]
        swap_copy(index).wait()

        @pl.loop(1, nears)
        def _(step):
            target = (near + step) % nears
            parts[parity, target] = add_up(parts[parity, target], arriving[target])
            near_copy(index, near, target).start()

    start_near(0)
    for turn in range(1, HALVES):
        target = (half + turn) % HALVES
        node_half[target] = gather_node(target).astype(jnp.bfloat16)
        far_copy(half, target).start()
    start_near(1)
    send_nodes(half)

    for index, (parts, arriving, close, _, _) in enumerate(chunks):

        def take_near(step, running):
            source = (near + nears - step) % nears
            near_copy(index, source, source).wait_recv()
            return running + close[source].astype(jnp.float32)

        running = parts[parity, near].astype(jnp.float32) + arriving[near].astype(jnp.float32)
        for step in range(1, nears):
            running = take_near(step, running)
        parts[parity, near] = running.astype(jnp.bfloat16)

        @pl.loop(1, lines)
        def _(step):
            line_copy(index, line, (line + step) % lines).start()

    for index, (parts, _, _, arriving, total) in enumerate(chunks):

        def take_line(step, running):
            source = (line + lines - step) % lines
            line_copy(index, source, source).wait_recv()
            return running + arriving[source].astype(jnp.float32)

        running = parts[parity, near, line].astype(jnp.float32)
        running = lax.fori_loop(1, lines, take_line, running)
        total[parity, near, line] = running.astype(jnp.bfloat16)

        @pl.loop(1, lines)
        def _(step):
            back_copy(index, line, (line + step) % lines).start()

    for index in range(2):

        @pl.loop(1, lines)
        def _(step):
            source = (line + lines - step) % lines
            back_copy(index, source, source).wait_recv()

        @pl.loop(1, nears)
        def _(step):
            wide_copy(index, near, (near + step) % nears).start()

        pass_copy(index, near, parity).start()

    running = gather_node(half)
    for turn in range(1, HALVES):
        source = (half + HALVES - turn) % HALVES
        far_copy(source, source).wait_recv()
        running = running + node_far[source].astype(jnp.float32)
    node_ref[...] = times_transpose(running.astype(jnp.bfloat16), w_mesh_ref[...]).astype(
        jnp.bfloat16
    )

    for index in range(2):

        @pl.loop(1, nears)
        def _(step):
            source = (near + nears - step) % nears
            wide_copy(index, source, source).wait_recv()
            pass_copy(index, source, parity).start()

    for index in range(2):

        @pl.loop(0, nears)
        def _(source):
            pass_copy(index, source, other).wait_recv()
            pass_copy(index, source, parity).wait_send()

        @pl.loop(1, nears)
        def _(step):
            near_copy(index, near, (near + step) % nears).wait_send()
            wide_copy(index, near, (near + step) % nears).wait_send()

        @pl.loop(1, lines)
        def _(step):
            line_copy(index, line, (line + step) % lines).wait_send()
            back_copy(index, line, (line + step) % lines).wait_send()

    @pl.loop(0, HALVES * lows)
    def _(count):
        part, step = split(count)

        @pl.when(step > 0)
        def _():
            point_copy(low, low_ahead(step), part).wait_send()

    for step in range(1, HALVES):
        half_copy(half, (half + step) % HALVES).wait_send()
        far_copy(half, (half + step) % HALVES).wait_send()
    for source_half in range(HALVES):
        for step in range(1, pairs):
            pair_copy(block_ref, source_half, pair, (pair + step) % pairs).wait_send()
            last_copy(source_half, pair, (pair + step) % pairs).wait_send()
        for source_pair in range(pairs):
            twin_copy(block_ref, source_half, 2 * source_pair + parity).wait_send()

    @pl.loop(1, group)
    def _(step):
        other_half, other_sub = member(step)
        edge_copy(half, sub, other_half, other_sub).wait_send()


def edge_pass(slots, latent, weighted, block, edges, w_mesh, w_grid, w_msg, w_out, capacity):
    bands, subs = lax.axis_size("band"), lax.axis_size("sub")
    lows, pairs = bands // HALVES, subs // 2
    nears, lines = 2 * pairs, bands // 2
    padded = round_up(subs * capacity, TILE)
    block_rows, width = block.shape
    patch = subs * block_rows
    columns = round_up(weighted.shape[0], LANES)
    lanes = round_up(padded, LANES)
    rows = width // (2 * nears * lines)
    vmem = pl.BlockSpec(memory_space=pltpu.VMEM)
    dma = pltpu.SemaphoreType.DMA
    half, full = jnp.bfloat16, jnp.float32

    def chunk(size):
        return [
            pltpu.VMEM((2, nears, lines, rows, size), half),
            pltpu.VMEM((nears, lines, rows, size), half),
            pltpu.VMEM((nears, lines, rows, size), half),
            pltpu.VMEM((lines, rows, size), half),
        ]

    return pl.pallas_call(
        functools.partial(edge_kernel, bands, subs, capacity),
        out_shape=(
            jax.ShapeDtypeStruct((block_rows, width), half),
            jax.ShapeDtypeStruct((2, nears, lines, rows, width + columns), half),
            jax.ShapeDtypeStruct((2, nears, lines, rows, width), half),
        ),
        in_specs=[vmem] * 9,
        out_specs=(vmem, vmem, vmem),
        scratch_shapes=[
            pltpu.VMEM((latent.shape[0], width + columns), half),
            pltpu.VMEM((columns, latent.shape[0]), half),
            pltpu.VMEM((width, columns), half),
            pltpu.VMEM((lows, HALVES, padded, width + columns), half),
            pltpu.VMEM((lows, HALVES, padded, width + columns), half),
            pltpu.VMEM((HALVES, subs, block_rows, width), half),
            pltpu.VMEM((HALVES, patch, width), half),
            pltpu.VMEM(edges.shape, jnp.int32),
            pltpu.VMEM((lows, HALVES, lanes, LANES), jnp.int32),
            pltpu.VMEM((columns, width), half),
            pltpu.VMEM((2, 3 * padded, patch), half),
            pltpu.VMEM((3 * padded, width), full),
            pltpu.VMEM((padded, width), half),
            pltpu.VMEM((padded, width), full),
            pltpu.VMEM((padded, width), half),
            pltpu.VMEM((2, 3 * padded, width), half),
            pltpu.VMEM((padded, width), half),
            pltpu.VMEM((HALVES, patch, width), full),
            pltpu.VMEM((width, width), full),
            pltpu.VMEM((width, columns), full),
            pltpu.VMEM((HALVES, subs, block_rows, width), half),
        ]
        + [pltpu.VMEM((HALVES, pairs, block_rows, width), half)] * 3
        + [pltpu.VMEM((HALVES, block_rows, width), half)] * 2
        + chunk(width + columns)
        + chunk(width)
        + [dma((lows, HALVES))] * 2
        + [
            dma((HALVES,)),
            dma((HALVES, pairs)),
            dma((HALVES, pairs)),
            dma((HALVES, subs)),
            dma((HALVES, subs)),
            dma((HALVES, subs)),
        ]
        + [dma((HALVES, pairs))] * 4
        + [dma((HALVES,))] * 2
        + [dma((2,))] * 2
        + [dma((2, nears))] * 2
        + [dma((2, lines))] * 4
        + [dma((2, nears))] * 4,
        compiler_params=pltpu.CompilerParams(
            collective_id=0, has_side_effects=True, vmem_limit_bytes=64000000
        ),
    )(slots, latent, weighted, block, edges, w_mesh, w_grid, w_msg, w_out)


def shards(grad_pred, grid_latent, mesh_latent, send_slot, edge_src, w_mesh, w_grid, w_msg, w_out):
    both = ("band", "sub")
    grid_rows, width = grid_latent.shape
    channels = grad_pred.shape[0]
    bands, subs = lax.axis_size("band"), lax.axis_size("sub")
    devices = bands * subs
    lows = bands // HALVES
    block_rows = mesh_latent.shape[0]
    capacity = 3 * grid_rows // devices
    padded = round_up(subs * capacity, TILE)
    total_points = grid_rows * devices
    own_index = lax.axis_index(both)
    points = own_index * grid_rows + jnp.arange(grid_rows, dtype=jnp.int32)
    weighted = (
        latitude_weight(points, total_points)[None, :] * grad_pred.astype(jnp.float32)
    ).astype(jnp.bfloat16)
    holder, rank = send_slot // capacity, send_slot % capacity
    holder_band, holder_sub = holder // subs, holder % subs
    holder_half, holder_low = holder_band // lows, holder_band % lows
    slots = (holder_low * HALVES + holder_half) * padded + holder_sub * capacity + rank
    local = edge_src - lax.axis_index("band") * (subs * block_rows)
    local = local.reshape(3, HALVES, lows, subs, capacity).transpose(1, 3, 2, 0, 4)
    local = local.reshape(HALVES, subs, 3 * lows, capacity)
    local = jnp.pad(local, ((0, 0), (0, 0), (0, -3 * lows % 8), (0, LANES - capacity)))
    mesh_grad, outer, inner = edge_pass(
        slots[None, :],
        grid_latent,
        weighted,
        mesh_latent,
        local,
        w_mesh,
        w_grid,
        w_msg,
        w_out,
        capacity,
    )
    grad_scale = 1.0 / math.sqrt(3.0 * total_points)
    outer = outer.reshape(width, outer.shape[-1])
    inner = inner.reshape(width, width)
    channel_part = outer[:, width:]
    return (
        mesh_grad,
        inner.astype(jnp.float32) * grad_scale,
        outer[:, :width].astype(jnp.float32) * grad_scale,
        times_transpose(channel_part[:, :channels], w_out) * grad_scale,
        contract_rows(w_msg, channel_part[:, :channels]) * grad_scale,
    )


def solution(mesh):
    placed = (
        P(None, ("band", "sub")),
        P(("band", "sub"), None),
        P(("band", "sub"), None),
        P(("band", "sub")),
        P(None, ("band", "sub")),
        P(),
        P(),
        P(),
        P(),
    )
    return jax.shard_map(
        shards,
        mesh=mesh,
        in_specs=placed,
        out_specs=(P(("band", "sub"), None), P(), P(), P(), P()),
        check_vma=False,
    )
```

```python
import functools
import math

import jax
import jax.numpy as jnp
from jax import lax
from jax.experimental import pallas as pl
from jax.experimental.pallas import tpu as pltpu
from jax.sharding import PartitionSpec as P

HALVES = 2
LANES = 128
TILE = 16
SPAN = 256


def latitude_weight(points, total):
    angle = jnp.pi * ((points.astype(jnp.float32) + 0.5) / total - 0.5)
    return 0.5 * jnp.pi * jnp.cos(angle)


def contract_rows(left, right):
    return lax.dot_general(
        left, right, (((0,), (0,)), ((), ())), preferred_element_type=jnp.float32
    )


def times_transpose(left, right):
    return lax.dot_general(
        left, right, (((1,), (1,)), ((), ())), preferred_element_type=jnp.float32
    )


def times(left, right):
    return jnp.dot(left, right, preferred_element_type=jnp.float32)


def round_up(value, multiple):
    return -(-value // multiple) * multiple


def remote(src, dst, send_sem, recv_sem, band, sub):
    return pltpu.make_async_remote_copy(
        src_ref=src,
        dst_ref=dst,
        send_sem=send_sem,
        recv_sem=recv_sem,
        device_id=(band, sub),
        device_id_type=pl.DeviceIdType.MESH,
    )


def greet(band, sub):
    pl.semaphore_signal(
        pltpu.get_barrier_semaphore(),
        inc=1,
        device_id=(band, sub),
        device_id_type=pl.DeviceIdType.MESH,
    )


def edge_kernel(
    bands,
    subs,
    capacity,
    slot_ref,
    latent_ref,
    weighted_ref,
    block_ref,
    edge_ref,
    w_mesh_ref,
    w_grid_ref,
    w_msg_ref,
    w_out_ref,
    node_ref,
    outer_ref,
    inner_ref,
    cargo,
    weighted,
    w_out,
    rows_out,
    rows_in,
    table,
    proj,
    edge_in,
    index_cols,
    act_weight,
    hot,
    pre,
    grid_part,
    act_grad,
    act_sum,
    pre_grad,
    grid_grad,
    node_acc,
    grid_acc,
    out_acc,
    node_out,
    node_in,
    node_sum,
    node_last,
    node_half,
    node_far,
    outer_parts,
    outer_in,
    outer_near,
    outer_line,
    inner_parts,
    inner_in,
    inner_near,
    inner_line,
    rows_send,
    rows_recv,
    half_send,
    pair_send,
    twin_send,
    table_recv,
    edge_send,
    edge_recv,
    node_send,
    node_recv,
    last_send,
    last_recv,
    far_send,
    far_recv,
    swap_send,
    swap_recv,
    near_send,
    near_recv,
    line_send,
    line_recv,
    back_send,
    back_recv,
    wide_send,
    wide_recv,
    pass_send,
    pass_recv,
):
    lows = bands // HALVES
    pairs = subs // 2
    nears = 2 * pairs
    lines = bands // 2
    padded = rows_out.shape[2]
    block_rows, width = block_ref.shape
    patch = subs * block_rows
    points = latent_ref.shape[0]
    band, sub = lax.axis_index("band"), lax.axis_index("sub")
    half, low = band // lows, band % lows
    pair, parity = sub // 2, sub % 2
    other = 1 - parity
    twin = 2 * pair + other
    group = HALVES * subs
    mine = half * subs + sub
    near, line = (band % 2) * pairs + pair, band // 2

    def low_ahead(step):
        return (low // 2 + step // 2) % (lows // 2) * 2 + (low % 2 + step % 2) % 2

    def low_behind(step):
        return (low // 2 + lows // 2 - step // 2) % (lows // 2) * 2 + (low % 2 + step % 2) % 2

    def member(step):
        index = (mine + step) % group
        return index // subs, index % subs

    def near_device(index):
        return line * 2 + index // pairs, 2 * (index % pairs) + parity

    def line_device(index):
        return index * 2 + band % 2, sub

    @pl.loop(1, group)
    def _(step):
        other_half, other_sub = member(step)
        greet(other_half * lows + low, other_sub)

    @pl.loop(1, lows)
    def _(step):
        greet(half * lows + low_ahead(step), sub)

    @pl.loop(1, nears)
    def _(step):
        greet(*near_device((near + step) % nears))

    @pl.loop(1, lines)
    def _(step):
        greet(*line_device((line + step) % lines))

    pl.semaphore_wait(
        pltpu.get_barrier_semaphore(), group - 1 + lows - 1 + nears - 1 + lines - 1
    )

    def half_copy(source, target):
        return remote(
            block_ref,
            table.at[source, sub],
            half_send.at[target],
            table_recv.at[source, sub],
            target * lows + low,
            sub,
        )

    def pair_copy(src, source_half, source, target):
        place = 2 * source + parity
        return remote(
            src,
            table.at[source_half, place],
            pair_send.at[source_half, target],
            table_recv.at[source_half, place],
            band,
            2 * target + parity,
        )

    def twin_copy(src, source_half, source):
        return remote(
            src,
            table.at[source_half, source],
            twin_send.at[source_half, source // 2],
            table_recv.at[source_half, source],
            band,
            twin,
        )

    def edge_copy(from_half, from_sub, to_half, to_sub):
        return remote(
            edge_ref.at[to_half, to_sub],
            edge_in.at[from_half, from_sub],
            edge_send.at[to_half, to_sub],
            edge_recv.at[from_half, from_sub],
            to_half * lows + low,
            to_sub,
        )

    @pl.loop(1, group)
    def _(step):
        other_half, other_sub = member(step)
        edge_copy(half, sub, other_half, other_sub).start()

    for step in range(1, pairs):
        pair_copy(block_ref, half, pair, (pair + step) % pairs).start()
    twin_copy(block_ref, half, sub).start()

    for step in range(1, HALVES):
        half_copy(half, (half + step) % HALVES).start()

    channels = weighted_ref.shape[0]
    weighted[...] = jnp.zeros_like(weighted)
    weighted[0:channels, :] = weighted_ref[...]
    cargo[:, 0:width] = latent_ref[...]
    cargo[:, width:] = weighted[...].astype(jnp.float32).T.astype(jnp.bfloat16)

    def spread(target, part, rows):
        places = lax.broadcasted_iota(jnp.int32, (padded, points), 0)
        places = places + (target * HALVES + part) * padded
        one_hot = jnp.where(places == slot_ref[...], 1.0, 0.0).astype(jnp.bfloat16)
        rows[target, part] = times(one_hot, cargo[...]).astype(jnp.bfloat16)

    def point_copy(source, target, part):
        return remote(
            rows_out.at[target, part],
            rows_in.at[source, part],
            rows_send.at[target, part],
            rows_recv.at[source, part],
            half * lows + target,
            sub,
        )

    def split(count):
        block = lows // 2
        turn = (count // block + 1) // 2
        return (half + turn) % HALVES, count - block * turn

    @pl.loop(0, HALVES * lows)
    def _(count):
        part, step = split(count)

        @pl.when(step > 0)
        def _():
            target = low_ahead(step)
            spread(target, part, rows_out)
            point_copy(low, target, part).start()

    for part in range(HALVES):
        spread(low, part, rows_in)

    table[half, sub] = block_ref[...]
    edge_in[half, sub] = edge_ref[half, sub]
    w_out[...] = jnp.zeros_like(w_out)
    w_out[:, 0:channels] = w_out_ref[...]
    act_weight[...] = 0.5 * lax.dot_general(
        w_out[...], w_msg_ref[...], (((0,), (1,)), ((), ())), preferred_element_type=jnp.float32
    ).astype(jnp.bfloat16)
    node_acc[...] = jnp.zeros_like(node_acc)
    grid_acc[...] = jnp.zeros_like(grid_acc)
    out_acc[...] = jnp.zeros_like(out_acc)

    def arrived(source_half, source):
        remote(
            block_ref,
            table.at[source_half, source],
            twin_send.at[0, 0],
            table_recv.at[source_half, source],
            band,
            twin,
        ).wait_recv()

    def project(source_half, source):
        rows = pl.ds(pl.multiple_of(source * block_rows, block_rows), block_rows)
        proj[source_half, rows] = 0.5 * times(
            table[source_half, source], w_mesh_ref[...]
        ).astype(jnp.bfloat16)

    def pass_pairs(source_half):
        for step in range(1, pairs):
            source = 2 * ((pair + step) % pairs) + parity
            arrived(source_half, source)
            twin_copy(table.at[source_half, source], source_half, source).start()

    def finish_table(source_half):
        for source_pair in range(pairs):
            arrived(source_half, 2 * source_pair + other)

        @pl.loop(0, subs)
        def _(source):
            project(source_half, source)

    pass_pairs(half)

    @pl.loop(1, group)
    def _(step):
        other_half, other_sub = member(step)
        edge_copy(other_half, other_sub, half, sub).wait_recv()

    lanes = index_cols.shape[2]
    count = edge_ref.shape[2]
    for part in range(HALVES):
        total = jnp.zeros((count, lanes), jnp.int32)
        for source in range(subs):
            piece = edge_in[part, source]
            if lanes > LANES:
                piece = jnp.concatenate(
                    [piece, jnp.zeros((count, lanes - LANES), jnp.int32)], axis=1
                )
            if source:
                piece = pltpu.roll(piece, source * capacity, 1)
            total = total + piece
        if count < LANES:
            total = jnp.concatenate([total, jnp.zeros((LANES - count, lanes), jnp.int32)], axis=0)
        flipped = total.T
        for source in range(lows):
            moved = pltpu.roll(flipped, LANES - 3 * source, 1) if source else flipped
            index_cols[source, part] = moved

    finish_table(half)

    for turn in range(1, HALVES):
        source_half = (half + turn) % HALVES
        arrived(source_half, sub)
        place = table.at[source_half, sub]
        twin_copy(place, source_half, sub).start()
        for index in range(1, pairs):
            pair_copy(place, source_half, pair, (pair + index) % pairs).start()

    def scatter(count, block):
        part, _ = split(count)
        slot = count % 2
        nodes = slice(block * SPAN, (block + 1) * SPAN)
        node_acc[part, nodes] += contract_rows(hot[slot, :, nodes], pre_grad[slot])

    def process(count, scattered):
        part, step = split(count)
        source = low_behind(step)
        slot = count % 2
        for corner in range(3):
            column = index_cols[source, part, 0:padded, corner : corner + 1]
            nodes = lax.broadcasted_iota(jnp.int32, (padded, patch), 1)
            hot[slot, corner * padded : (corner + 1) * padded, :] = jnp.where(
                nodes == column, 1.0, 0.0
            ).astype(jnp.bfloat16)
        latents = rows_in[source, part, :, 0:width]
        losses = rows_in[source, part, :, width:]
        pre[...] = times(hot[slot], proj[part])
        grid_part[...] = 0.5 * times(latents, w_grid_ref[...]).astype(jnp.bfloat16)
        act_grad[...] = times(losses, act_weight[...])

        def finish(start):
            rows = pl.ds(start, TILE)
            base = grid_part[rows].astype(jnp.float32)
            upper = act_grad[rows]
            acts, grads = None, None
            for corner in range(3):
                place = pl.ds(corner * padded + start, TILE)
                value = pre[place] + base
                tanh = jnp.tanh(value)
                above = 1.0 + tanh
                act = value * above
                grad = upper * (above + act * (1.0 - tanh))
                pre_grad[slot, place] = grad.astype(jnp.bfloat16)
                acts = act if acts is None else acts + act
                grads = grad if grads is None else grads + grad
            act_sum[rows] = acts.astype(jnp.bfloat16)
            grid_grad[rows] = grads.astype(jnp.bfloat16)

        tiles = padded // TILE
        blocks = patch // SPAN
        done = 0
        for tile in range(tiles):
            while scattered and done * tiles < (tile + 1) * blocks:
                scatter(count - 1, done)
                done += 1
            finish(tile * TILE)

        out_acc[...] += contract_rows(act_sum[...], losses)
        grid_acc[...] += contract_rows(latents, grid_grad[...])

    def node_copies(part):
        return [
            remote(
                node_out.at[part, 2 * index + other],
                node_in.at[part, index],
                node_send.at[part, index],
                node_recv.at[part, index],
                band,
                twin,
            )
            for index in range(pairs)
        ]

    def last_copy(part, source, target):
        return remote(
            node_sum.at[part, target],
            node_last.at[part, source],
            last_send.at[part, target],
            last_recv.at[part, source],
            band,
            2 * target + parity,
        )

    def far_copy(source, target):
        return remote(
            node_half.at[target],
            node_far.at[source],
            far_send.at[target],
            far_recv.at[source],
            target * lows + low,
            sub,
        )

    def add_node(part, index):
        return node_out[part, 2 * index + parity].astype(jnp.float32) + node_in[
            part, index
        ].astype(jnp.float32)

    def swap_nodes(part):
        for source in range(subs):
            rows = pl.ds(source * block_rows, block_rows)
            node_out[part, source] = node_acc[part, rows].astype(jnp.bfloat16)
        for copy in node_copies(part):
            copy.start()

    def send_nodes(part):
        for copy in node_copies(part):
            copy.wait()
        for step in range(1, pairs):
            target = (pair + step) % pairs
            node_sum[part, target] = add_node(part, target).astype(jnp.bfloat16)
            last_copy(part, pair, target).start()

    def gather_node(part):
        running = add_node(part, pair)
        for step in range(1, pairs):
            source = (pair + pairs - step) % pairs
            last_copy(part, source, source).wait_recv()
            running = running + node_last[part, source].astype(jnp.float32)
        return running

    def scatter_all(count):
        for block in range(patch // SPAN):
            scatter(count, block)

    def run(count):
        part, step = split(count)
        source = low_behind(step)

        @pl.when(step > 0)
        def _():
            point_copy(source, source, part).wait_recv()

        process(count, True)

    first = lows // 2
    last = first + (HALVES - 1) * lows

    process(0, False)
    @pl.loop(1, first)
    def _(count):
        run(count)

    for turn in range(1, HALVES):
        pass_pairs((half + turn) % HALVES)
        finish_table((half + turn) % HALVES)

    @pl.loop(first, last)
    def _(count):
        run(count)

    scatter_all(last - 1)
    for turn in range(1, HALVES):
        swap_nodes((half + turn) % HALVES)
    part, step = split(last)
    source = low_behind(step)
    point_copy(source, source, part).wait_recv()
    process(last, False)
    for turn in range(1, HALVES):
        send_nodes((half + turn) % HALVES)

    @pl.loop(last + 1, HALVES * lows)
    def _(count):
        run(count)

    chunks = (
        (outer_parts, outer_in, outer_near, outer_line, outer_ref),
        (inner_parts, inner_in, inner_near, inner_line, inner_ref),
    )

    def swap_copy(index):
        parts, arriving = chunks[index][:2]
        return remote(
            parts.at[other], arriving, swap_send.at[index], swap_recv.at[index], band, twin
        )

    def near_copy(index, source, target):
        parts, _, arriving = chunks[index][:3]
        return remote(
            parts.at[parity, target],
            arriving.at[source],
            near_send.at[index, target],
            near_recv.at[index, source],
            *near_device(target),
        )

    def line_copy(index, source, target):
        parts, _, _, arriving = chunks[index][:4]
        return remote(
            parts.at[parity, near, target],
            arriving.at[source],
            line_send.at[index, target],
            line_recv.at[index, source],
            *line_device(target),
        )

    def back_copy(index, source, target):
        place = chunks[index][4].at[parity, near, source]
        return remote(
            place,
            place,
            back_send.at[index, target],
            back_recv.at[index, source],
            *line_device(target),
        )

    def wide_copy(index, source, target):
        place = chunks[index][4].at[parity, source]
        return remote(
            place,
            place,
            wide_send.at[index, target],
            wide_recv.at[index, source],
            *near_device(target),
        )

    def pass_copy(index, source, side):
        place = chunks[index][4].at[side, source]
        return remote(
            place, place, pass_send.at[index, source], pass_recv.at[index, source], band, twin
        )

    rows = outer_parts.shape[3]

    def fill(parts, value, first):
        for device in range(nears * lines * 2):
            place = (device // (nears * lines), device // lines % nears, device % lines)
            piece = value[device * rows : (device + 1) * rows]
            parts[place + (slice(None), slice(first, first + value.shape[1]))] = piece.astype(
                jnp.bfloat16
            )

    fill(outer_parts, grid_acc[...], 0)
    fill(outer_parts, out_acc[...], width)
    swap_copy(0).start()
    scatter_all(HALVES * lows - 1)
    swap_nodes(half)
    for turn in range(1, HALVES):
        target = (half + turn) % HALVES
        node_half[target] = gather_node(target).astype(jnp.bfloat16)
        far_copy(half, target).start()
    mesh_total = None
    for part in range(HALVES):
        for source in range(subs):
            term = contract_rows(table[part, source], node_out[part, source])
            mesh_total = term if mesh_total is None else mesh_total + term
    fill(inner_parts, mesh_total, 0)
    swap_copy(1).start()

    def add_up(left, right):
        return (left.astype(jnp.float32) + right.astype(jnp.float32)).astype(jnp.bfloat16)

    def start_near(index):
        parts, arriving = chunks[index][:2]
        swap_copy(index).wait()

        @pl.loop(1, nears)
        def _(step):
            target = (near + step) % nears
            parts[parity, target] = add_up(parts[parity, target], arriving[target])
            near_copy(index, near, target).start()

    start_near(0)
    start_near(1)
    send_nodes(half)

    for index, (parts, arriving, close, _, _) in enumerate(chunks):

        def take_near(step, running):
            source = (near + nears - step) % nears
            near_copy(index, source, source).wait_recv()
            return running + close[source].astype(jnp.float32)

        running = parts[parity, near].astype(jnp.float32) + arriving[near].astype(jnp.float32)
        for step in range(1, nears):
            running = take_near(step, running)
        parts[parity, near] = running.astype(jnp.bfloat16)

        @pl.loop(1, lines)
        def _(step):
            line_copy(index, line, (line + step) % lines).start()

    for index, (parts, _, _, arriving, total) in enumerate(chunks):

        def take_line(step, running):
            source = (line + lines - step) % lines
            line_copy(index, source, source).wait_recv()
            return running + arriving[source].astype(jnp.float32)

        running = parts[parity, near, line].astype(jnp.float32)
        running = lax.fori_loop(1, lines, take_line, running)
        total[parity, near, line] = running.astype(jnp.bfloat16)

        @pl.loop(1, lines)
        def _(step):
            back_copy(index, line, (line + step) % lines).start()

    for index in range(2):

        @pl.loop(1, lines)
        def _(step):
            source = (line + lines - step) % lines
            back_copy(index, source, source).wait_recv()

        @pl.loop(1, nears)
        def _(step):
            wide_copy(index, near, (near + step) % nears).start()

        pass_copy(index, near, parity).start()

    running = gather_node(half)
    for turn in range(1, HALVES):
        source = (half + HALVES - turn) % HALVES
        far_copy(source, source).wait_recv()
        running = running + node_far[source].astype(jnp.float32)
    node_ref[...] = times_transpose(running.astype(jnp.bfloat16), w_mesh_ref[...]).astype(
        jnp.bfloat16
    )

    for index in range(2):

        @pl.loop(1, nears)
        def _(step):
            source = (near + nears - step) % nears
            wide_copy(index, source, source).wait_recv()
            pass_copy(index, source, parity).start()

    for index in range(2):

        @pl.loop(0, nears)
        def _(source):
            pass_copy(index, source, other).wait_recv()
            pass_copy(index, source, parity).wait_send()

        @pl.loop(1, nears)
        def _(step):
            near_copy(index, near, (near + step) % nears).wait_send()
            wide_copy(index, near, (near + step) % nears).wait_send()

        @pl.loop(1, lines)
        def _(step):
            line_copy(index, line, (line + step) % lines).wait_send()
            back_copy(index, line, (line + step) % lines).wait_send()

    @pl.loop(0, HALVES * lows)
    def _(count):
        part, step = split(count)

        @pl.when(step > 0)
        def _():
            point_copy(low, low_ahead(step), part).wait_send()

    for step in range(1, HALVES):
        half_copy(half, (half + step) % HALVES).wait_send()
        far_copy(half, (half + step) % HALVES).wait_send()
    for source_half in range(HALVES):
        for step in range(1, pairs):
            pair_copy(block_ref, source_half, pair, (pair + step) % pairs).wait_send()
            last_copy(source_half, pair, (pair + step) % pairs).wait_send()
        for source_pair in range(pairs):
            twin_copy(block_ref, source_half, 2 * source_pair + parity).wait_send()

    @pl.loop(1, group)
    def _(step):
        other_half, other_sub = member(step)
        edge_copy(half, sub, other_half, other_sub).wait_send()


def edge_pass(slots, latent, weighted, block, edges, w_mesh, w_grid, w_msg, w_out, capacity):
    bands, subs = lax.axis_size("band"), lax.axis_size("sub")
    lows, pairs = bands // HALVES, subs // 2
    nears, lines = 2 * pairs, bands // 2
    padded = round_up(subs * capacity, TILE)
    block_rows, width = block.shape
    patch = subs * block_rows
    columns = round_up(weighted.shape[0], LANES)
    lanes = round_up(padded, LANES)
    rows = width // (2 * nears * lines)
    vmem = pl.BlockSpec(memory_space=pltpu.VMEM)
    dma = pltpu.SemaphoreType.DMA
    half, full = jnp.bfloat16, jnp.float32

    def chunk(size):
        return [
            pltpu.VMEM((2, nears, lines, rows, size), half),
            pltpu.VMEM((nears, lines, rows, size), half),
            pltpu.VMEM((nears, lines, rows, size), half),
            pltpu.VMEM((lines, rows, size), half),
        ]

    return pl.pallas_call(
        functools.partial(edge_kernel, bands, subs, capacity),
        out_shape=(
            jax.ShapeDtypeStruct((block_rows, width), half),
            jax.ShapeDtypeStruct((2, nears, lines, rows, width + columns), half),
            jax.ShapeDtypeStruct((2, nears, lines, rows, width), half),
        ),
        in_specs=[vmem] * 9,
        out_specs=(vmem, vmem, vmem),
        scratch_shapes=[
            pltpu.VMEM((latent.shape[0], width + columns), half),
            pltpu.VMEM((columns, latent.shape[0]), half),
            pltpu.VMEM((width, columns), half),
            pltpu.VMEM((lows, HALVES, padded, width + columns), half),
            pltpu.VMEM((lows, HALVES, padded, width + columns), half),
            pltpu.VMEM((HALVES, subs, block_rows, width), half),
            pltpu.VMEM((HALVES, patch, width), half),
            pltpu.VMEM(edges.shape, jnp.int32),
            pltpu.VMEM((lows, HALVES, lanes, LANES), jnp.int32),
            pltpu.VMEM((columns, width), half),
            pltpu.VMEM((2, 3 * padded, patch), half),
            pltpu.VMEM((3 * padded, width), full),
            pltpu.VMEM((padded, width), half),
            pltpu.VMEM((padded, width), full),
            pltpu.VMEM((padded, width), half),
            pltpu.VMEM((2, 3 * padded, width), half),
            pltpu.VMEM((padded, width), half),
            pltpu.VMEM((HALVES, patch, width), full),
            pltpu.VMEM((width, width), full),
            pltpu.VMEM((width, columns), full),
            pltpu.VMEM((HALVES, subs, block_rows, width), half),
        ]
        + [pltpu.VMEM((HALVES, pairs, block_rows, width), half)] * 3
        + [pltpu.VMEM((HALVES, block_rows, width), half)] * 2
        + chunk(width + columns)
        + chunk(width)
        + [dma((lows, HALVES))] * 2
        + [
            dma((HALVES,)),
            dma((HALVES, pairs)),
            dma((HALVES, pairs)),
            dma((HALVES, subs)),
            dma((HALVES, subs)),
            dma((HALVES, subs)),
        ]
        + [dma((HALVES, pairs))] * 4
        + [dma((HALVES,))] * 2
        + [dma((2,))] * 2
        + [dma((2, nears))] * 2
        + [dma((2, lines))] * 4
        + [dma((2, nears))] * 4,
        compiler_params=pltpu.CompilerParams(
            collective_id=0, has_side_effects=True, vmem_limit_bytes=64000000
        ),
    )(slots, latent, weighted, block, edges, w_mesh, w_grid, w_msg, w_out)


def shards(grad_pred, grid_latent, mesh_latent, send_slot, edge_src, w_mesh, w_grid, w_msg, w_out):
    both = ("band", "sub")
    grid_rows, width = grid_latent.shape
    channels = grad_pred.shape[0]
    bands, subs = lax.axis_size("band"), lax.axis_size("sub")
    devices = bands * subs
    lows = bands // HALVES
    block_rows = mesh_latent.shape[0]
    capacity = 3 * grid_rows // devices
    padded = round_up(subs * capacity, TILE)
    total_points = grid_rows * devices
    own_index = lax.axis_index(both)
    points = own_index * grid_rows + jnp.arange(grid_rows, dtype=jnp.int32)
    weighted = (
        latitude_weight(points, total_points)[None, :] * grad_pred.astype(jnp.float32)
    ).astype(jnp.bfloat16)
    holder, rank = send_slot // capacity, send_slot % capacity
    holder_band, holder_sub = holder // subs, holder % subs
    holder_half, holder_low = holder_band // lows, holder_band % lows
    slots = (holder_low * HALVES + holder_half) * padded + holder_sub * capacity + rank
    local = edge_src - lax.axis_index("band") * (subs * block_rows)
    local = local.reshape(3, HALVES, lows, subs, capacity).transpose(1, 3, 2, 0, 4)
    local = local.reshape(HALVES, subs, 3 * lows, capacity)
    local = jnp.pad(local, ((0, 0), (0, 0), (0, -3 * lows % 8), (0, LANES - capacity)))
    mesh_grad, outer, inner = edge_pass(
        slots[None, :],
        grid_latent,
        weighted,
        mesh_latent,
        local,
        w_mesh,
        w_grid,
        w_msg,
        w_out,
        capacity,
    )
    grad_scale = 1.0 / math.sqrt(3.0 * total_points)
    outer = outer.reshape(width, outer.shape[-1])
    inner = inner.reshape(width, width)
    channel_part = outer[:, width:]
    return (
        mesh_grad,
        inner.astype(jnp.float32) * grad_scale,
        outer[:, :width].astype(jnp.float32) * grad_scale,
        times_transpose(channel_part[:, :channels], w_out) * grad_scale,
        contract_rows(w_msg, channel_part[:, :channels]) * grad_scale,
    )


def solution(mesh):
    placed = (
        P(None, ("band", "sub")),
        P(("band", "sub"), None),
        P(("band", "sub"), None),
        P(("band", "sub")),
        P(None, ("band", "sub")),
        P(),
        P(),
        P(),
        P(),
    )
    return jax.shard_map(
        shards,
        mesh=mesh,
        in_specs=placed,
        out_specs=(P(("band", "sub"), None), P(), P(), P(), P()),
        check_vma=False,
    )
```
